512 devices in a mesh: replica: 32 (over y_hi, z), tp: 16 (over x, y_lo, core).
Axes of the slice: x: 4, y: 8 (y_hi: 4, y_lo: 2; y = y_hi * 2 + y_lo), z: 8, core: 2. Of those that a mesh axis runs over, the one named last changes fastest.
Arguments:
- hidden: bfloat16 [1536, 4, 8192], P('replica', None, 'tp'), may hold values from -6 to 6
- norm_gain: float32 [8192], replicated, may hold values from 0.5 to 1.5
- w_query: float32 [8192, 4096], P(('replica', 'tp')), may hold values from -0.0625 to 0.0625
- w_key: float32 [8192, 512], P(('replica', 'tp')), may hold values from -0.0625 to 0.0625
- w_value: float32 [8192, 512], P(('replica', 'tp')), may hold values from -0.0625 to 0.0625
- bias_query: float32 [4096], P('tp'), may hold values from -3 to 3
- bias_key: float32 [512], P('tp'), may hold values from -3 to 3
- bias_value: float32 [512], P('tp'), may hold values from -3 to 3
- key_pages: bfloat16 [8192, 4, 128, 128], P(('replica', 'tp')), may hold values from -256 to 256
- value_pages: bfloat16 [8192, 4, 128, 128], P(('replica', 'tp')), may hold values from -6 to 6
- kv_lengths: int32 [1536], P(('replica', 'tp')), may hold values from 1 to 1024, as said below
- page_table: int32 [1536, 8], P(('replica', 'tp')), may hold values from 0 to 15, as said below
Outputs:
- attended: bfloat16 [1536, 4, 4096], P(('replica', 'tp'))
The draws below stay inside these ranges and needn't reach their ends.
Inputs may be any that keep to these rules, and one draw needn't show every extreme that they name: `kv_lengths`: on every device, one row has exactly 1024 cached tokens. `page_table`: page ids are local to the pool of 16 pages of the device that holds the row. The first ceil(kv_lengths / 128) entries of a row name its pages in order; no page serves two of those entries on one device; later entries are arbitrary pages of the pool.
All inputs are finite; a program needn't handle non-finite values.
Results may differ from the reference program's by a relative error of at most 0.04.
Values may be sent and summed in bfloat16 or wider, within the bound.
A program may use at most 128 MiB of HBM per device.

```python
import jax
import jax.numpy as jnp
from jax import lax

D = 8192
HD = 128
HQ = 32
KVH = 4
STEPS = 4
PAGE = 128
MOSTP = 8
ROWS_DEV = 3
PAGES_DEV = 16
ROWS = 1536
NPAGES = 8192


def layout_device(key):
    keys = jax.random.split(key, 4)
    raw = jax.random.randint(keys[0], (ROWS_DEV,), 1, MOSTP + 1)
    chosen = jax.random.randint(keys[1], (), 0, ROWS_DEV)
    index = jnp.arange(ROWS_DEV, dtype=jnp.int32)
    longest = index == chosen

    def settle(used, item):
        value, is_long, place = item
        later = ROWS_DEV - 1 - place - (chosen > place).astype(jnp.int32)
        room = PAGES_DEV - MOSTP - used - later
        amount = jnp.where(is_long, MOSTP, jnp.minimum(value, room))
        return (used + jnp.where(is_long, 0, amount), amount)
    _, counts = lax.scan(settle, jnp.int32(0), (raw, longest, index))
    trims = jax.random.randint(keys[2], (ROWS_DEV,), 0, PAGE)
    trims = jnp.where(longest, 0, trims)
    lengths = counts * PAGE - trims
    order = jax.random.permutation(keys[3], PAGES_DEV).astype(jnp.int32)
    starts = jnp.cumsum(counts) - counts
    slots = (starts[:, None] + jnp.arange(MOSTP, dtype=jnp.int32)[None, :]) % PAGES_DEV
    table = order[slots]
    return (lengths.astype(jnp.int32), table.astype(jnp.int32))


def layout_all(key):
    base = jax.random.fold_in(key, 17)
    devices = ROWS // ROWS_DEV
    keys = jax.vmap(lambda d: jax.random.fold_in(base, d))(jnp.arange(devices))
    lengths, tables = jax.vmap(layout_device)(keys)
    return (lengths.reshape(ROWS), tables.reshape(ROWS, MOSTP))


def draw_kv_lengths(key, part):
    return layout_all(key)[0]


def draw_page_table(key, part):
    return layout_all(key)[1]


def draw_key_pages(key, part):
    first = jax.random.fold_in(jax.random.fold_in(key, 5), 0)
    base = jax.random.normal(first, (NPAGES, KVH, PAGE, HD), jnp.float32)
    base = jnp.clip(base, -6.0, 6.0)
    return base.astype(jnp.bfloat16)


def block_scale(rng, extent, cuts, smallest, largest):
    gain, own = 1.0, jax.random.fold_in(rng, 6)
    for position, blocks in cuts:
        heights = jnp.exp(jax.random.uniform(jax.random.fold_in(own, position), (blocks,), jnp.float32, smallest / len(cuts), largest / len(cuts)))
        gain = gain * jnp.repeat(heights, extent[position] // blocks).reshape([-1 if axis == position else 1 for axis in range(len(extent))])
    return gain


def gaussian(rng, shape, scale, most, cuts=(), held_as=jnp.bfloat16):
    array = jax.random.normal(rng, shape, jnp.float32) * scale
    if len(cuts) > 0:
        array = block_scale(rng, shape, cuts, -0.22, 0.18) * array
    return jnp.clip(array, min=-most, max=most).astype(held_as)


def setup_inputs(seed: int = 0) -> dict:
    streams_of = jax.random.split(jax.random.key(seed), 13)
    hidden = gaussian(streams_of[0], (ROWS, STEPS, D), 1.0, 6.0, ((0, 32), (2, 16)))
    norm_gain = jnp.clip(1.0 + 0.1 * jax.random.normal(streams_of[1], (D,), jnp.float32), 0.5, 1.5)
    w_query = gaussian(streams_of[2], (D, HQ * HD), D ** -0.5, 0.0625, ((0, 512),), jnp.float32)
    w_key = gaussian(streams_of[3], (D, KVH * HD), D ** -0.5, 0.0625, ((0, 512),), jnp.float32)
    w_value = gaussian(streams_of[4], (D, KVH * HD), D ** -0.5, 0.0625, ((0, 512),), jnp.float32)
    bias_query = gaussian(streams_of[5], (HQ * HD,), 0.5, 3.0, ((0, 16),), jnp.float32)
    bias_key = gaussian(streams_of[6], (KVH * HD,), 0.5, 3.0, ((0, 16),), jnp.float32)
    bias_value = gaussian(streams_of[7], (KVH * HD,), 0.5, 3.0, ((0, 16),), jnp.float32)
    key_pages = draw_key_pages(jax.random.fold_in(streams_of[12], 71), 0)
    value_pages = gaussian(streams_of[9], (NPAGES, KVH, PAGE, HD), 1.0, 6.0, ((0, 512),))
    kv_lengths = draw_kv_lengths(jax.random.fold_in(streams_of[12], 71), 0)
    page_table = draw_page_table(jax.random.fold_in(streams_of[12], 71), 0)
    return {"hidden": hidden, "norm_gain": norm_gain, "w_query": w_query, "w_key": w_key, "w_value": w_value, "bias_query": bias_query, "bias_key": bias_key, "bias_value": bias_value, "key_pages": key_pages, "value_pages": value_pages, "kv_lengths": kv_lengths, "page_table": page_table}


EPS = 1e-06
THETA = 1000000.0

def rotate(values, positions):
    half = values.shape[-1] // 2
    freq = THETA ** (-(jnp.arange(half, dtype=jnp.float32) * 2.0 / values.shape[-1]))
    angle = positions.astype(jnp.float32)[..., None] * freq
    angle = jnp.concatenate([angle, angle], -1)[:, :, None, :]
    turned = jnp.concatenate([-values[..., half:], values[..., :half]], -1)
    return values * jnp.cos(angle) + turned * jnp.sin(angle)

def reference(hidden, norm_gain, w_query, w_key, w_value, bias_query, bias_key, bias_value, key_pages, value_pages, kv_lengths, page_table):
    count, steps, width = hidden.shape
    wide = hidden.astype(jnp.float32)
    power = lax.optimization_barrier(jnp.mean(wide * wide, axis=2, keepdims=True))
    normed = (wide * lax.rsqrt(power + EPS) * norm_gain).astype(jnp.bfloat16).reshape(count * steps, width)

    def project(weight, bias):
        out = jnp.dot(normed, weight.astype(jnp.bfloat16), preferred_element_type=jnp.float32) + bias
        return out.astype(jnp.bfloat16)
    query = project(w_query, bias_query).reshape(count, steps, HQ, HD)
    key_new = project(w_key, bias_key).reshape(count, steps, KVH, HD)
    value_new = project(w_value, bias_value).reshape(count, steps, KVH, HD)
    positions = kv_lengths[:, None] + jnp.arange(steps, dtype=jnp.int32)[None, :]
    query_rot = rotate(query.astype(jnp.float32), positions).astype(jnp.bfloat16)
    key_rot = rotate(key_new.astype(jnp.float32), positions).astype(jnp.bfloat16)
    group = HQ // KVH
    scale = 1.0 / HD ** 0.5
    causal = jnp.arange(steps)[None, :] <= jnp.arange(steps)[:, None]

    def one_row(item):
        index, q_row, k_row, v_row, length, table = item
        device = index // ROWS_DEV
        ids = (device * PAGES_DEV + table).astype(jnp.int32)
        keys = key_pages[ids].astype(jnp.float32)
        vals = value_pages[ids].astype(jnp.float32)
        q5 = q_row.astype(jnp.float32).reshape(steps, KVH, group, HD)
        cache = jnp.einsum('tkgd,mknd->tkgmn', q5, keys) * scale
        spot = jnp.arange(MOSTP)[:, None] * PAGE + jnp.arange(PAGE)[None, :]
        live = (spot < length)[None, None, None]
        cache = jnp.where(live, cache, -1e+30)
        fresh = jnp.einsum('tkgd,skd->tkgs', q5, k_row.astype(jnp.float32)) * scale
        fresh = jnp.where(causal[:, None, None, :], fresh, -1e+30)
        top = jnp.maximum(lax.optimization_barrier(jnp.max(cache, axis=(3, 4))), lax.optimization_barrier(jnp.max(fresh, axis=3)))
        e_cache = jnp.where(live, jnp.exp(cache - top[..., None, None]), 0.0)
        e_fresh = jnp.where(causal[:, None, None, :], jnp.exp(fresh - top[..., None]), 0.0)
        total = lax.optimization_barrier(jnp.sum(e_cache, axis=(3, 4))) + lax.optimization_barrier(jnp.sum(e_fresh, axis=3))
        w_cache = (e_cache / total[..., None, None]).astype(jnp.bfloat16).astype(jnp.float32)
        w_fresh = (e_fresh / total[..., None]).astype(jnp.bfloat16).astype(jnp.float32)
        out = jnp.einsum('tkgmn,mknd->tkgd', w_cache, vals)
        out = out + jnp.einsum('tkgs,skd->tkgd', w_fresh, v_row.astype(jnp.float32))
        return out.reshape(steps, HQ * HD).astype(jnp.bfloat16)
    rows_index = jnp.arange(count, dtype=jnp.int32)
    return lax.map(one_row, (rows_index, query_rot, key_rot, value_new, kv_lengths, page_table))
```

```python
import functools

import jax
import jax.numpy as jnp
from jax import lax
from jax.experimental import pallas as pl
from jax.experimental.pallas import tpu as pltpu
from jax.sharding import Mesh
from jax.sharding import PartitionSpec as P

HD = 128
HQ = 32
KVH = 4
GROUP = HQ // KVH
PAGE = 128
MOSTP = 8
STEPS = 4
ROWS = 3
OWN = ROWS * STEPS
D = 8192
EPS = 1e-06
THETA = 1000000.0
MESH = pl.DeviceIdType.MESH
AXES = ("yh", "z", "x", "yl", "c")
TP = ("x", "yl", "c")
REPLICA = ("yh", "z")
COLS = 640
KB = 512
BR = 192
RT = 96


def remote(src, dst, send, recv, where):
    return pltpu.make_async_remote_copy(
        src_ref=src, dst_ref=dst, send_sem=send, recv_sem=recv, device_id=where, device_id_type=MESH
    )


def project_kernel(
    x_ref, w_ref, st_ref,
    out_ref, sto_ref,
    xg, a1, wz, acc, dsend, drecv, rsend, rrecv, fin, ysend, yrecv, strecv,
    xs, xr, a1s, a1r, a2s, a2r, ws, wr, sts, strs, d2s, d2r, rss, rrs, yss, yrs,
):
    yh, z, x, yl, c = (lax.axis_index(a) for a in AXES)
    y = yh * 2 + yl
    tp = x * 4 + yl * 2 + c
    zb = lax.rem(z // 2, 2)

    def at_y(k):
        return {"yh": k // 2, "yl": lax.rem(k, 2)}

    def at_tp(k):
        return {"x": k // 4, "yl": lax.rem(k // 2, 2), "c": lax.rem(k, 2)}

    def add(a, k, n):
        return lax.rem(a + (k + n) % n, n)

    barrier = pltpu.get_barrier_semaphore()
    for d in range(1, 16):
        pl.semaphore_signal(barrier, inc=1, device_id=at_tp(add(tp, d, 16)), device_id_type=MESH)
    for d in range(1, 4):
        for k in range(2):
            pl.semaphore_signal(
                barrier, inc=1, device_id={"yh": add(yh, d, 4), "yl": k}, device_id_type=MESH
            )
    for d in (1, -1):
        pl.semaphore_signal(barrier, inc=1, device_id={"z": add(z, d, 8)}, device_id_type=MESH)
    pl.semaphore_wait(barrier, 23)

    y_next = (at_y(add(y, 1, 8)), at_y(add(y, -1, 8)))
    z_next = ({"z": add(z, 1, 8)}, {"z": add(z, -1, 8)})

    def x_copy(s, h, way):
        o = add(y, -(s - 1) if way == 0 else s - 1, 8)
        rows = pl.ds(RT * h, RT)
        src = x_ref.at[rows] if s == 1 else xg.at[o, rows]
        return remote(
            src, xg.at[o, rows], xs.at[way, s - 1, h], xr.at[way, s - 1, h], y_next[way]
        )

    def x_wait(s, h, way):
        o = add(y, -s if way == 0 else s, 8)
        dst = xg.at[o, pl.ds(RT * h, RT)]
        remote(dst, dst, xs.at[way, s - 1, h], xr.at[way, s - 1, h], y_next[way]).wait_recv()

    def goes(s, h, way):
        return s <= 3 or (s == 4 and h == way)

    def origin_w(s, way):
        o = add(z, -s if way == 0 else s, 8)
        return o, lax.rem(o // 2, 2) == c, (o // 4) * 2 + lax.rem(o, 2)

    def w_copy(s, h, way):
        _, mine, j = origin_w(s - 1, way)
        part = wz.at[j, pl.ds(2 * h, 2)]
        return mine, remote(
            part, part, ws.at[way, s - 1, h], wr.at[way, s - 1, h], z_next[way]
        )

    def w_send(s, h, way):
        mine, copy = w_copy(s, h, way)

        @pl.when(mine)
        def _():
            copy.start()

    def w_step(s, h, way):
        _, mine, j = origin_w(s, way)
        part = wz.at[j, pl.ds(2 * h, 2)]

        @pl.when(mine)
        def _():
            remote(
                part, part, ws.at[way, s - 1, h], wr.at[way, s - 1, h], z_next[way]
            ).wait_recv()
            if goes(s + 1, h, way):
                w_copy(s + 1, h, way)[1].start()

    def x_step(s, h):
        for way in range(2):
            if goes(s, h, way):
                x_wait(s, h, way)
                if goes(s + 1, h, way):
                    x_copy(s + 1, h, way).start()

    def a1_copy(d):
        k = add(y, d, 8)
        return remote(w_ref.at[k], a1.at[y], a1s.at[d], a1r.at[y], at_y(k))

    for d in (4, 3, 5, 2, 6, 1, 7):
        a1_copy(d).start()
    for h in range(2):
        for way in range(2):
            x_copy(1, h, way).start()

    def st_copy(d):
        k = add(tp, d, 16)
        return remote(st_ref.at[k], strecv.at[tp], sts.at[d], strs.at[tp], at_tp(k))

    for d in range(1, 16):
        st_copy(d).start()
    a1[y] = w_ref[y]
    xg[y] = x_ref[...]
    strecv[tp] = st_ref[tp]

    for d in range(1, 8):
        k = add(y, d, 8)
        remote(a1.at[k], a1.at[k], a1s.at[d], a1r.at[k], at_y(k)).wait_recv()

    own_j = (z // 4) * 2 + lax.rem(z, 2)

    def a2_copy(d):
        k = add(x, d, 4)
        return remote(
            a1.at[pl.ds(2 * k, 2)],
            wz.at[own_j, x, :, c],
            a2s.at[d],
            a2r.at[x * 2 + c],
            {"x": k, "c": zb},
        )

    for d in (2, 1, 3):
        a2_copy(d).start()

    @pl.when(zb != c)
    def _():
        a2_copy(0).start()

    @pl.when(zb == c)
    def _():
        wz[own_j, x, :, c] = a1[pl.ds(2 * x, 2)]

    x_step(1, 0)
    x_step(1, 1)

    @pl.when(zb == c)
    def _():
        for d in range(8):
            k = add(x * 2 + c, d, 8)
            kx, kc = k // 2, lax.rem(k, 2)
            dst = wz.at[own_j, kx, :, kc]
            if d > 0:
                remote(dst, dst, a2s.at[0], a2r.at[k], {"x": kx, "c": kc}).wait_recv()

    for h in range(2):
        for way in range(2):
            w_send(1, h, way)
    x_step(2, 0)
    x_step(2, 1)
    for s in range(1, 5):
        for h in range(2):
            for way in range(2):
                if goes(s, h, way):
                    w_step(s, h, way)
        if s == 1:
            x_step(3, 0)
            x_step(3, 1)
        if s == 2:
            x_step(4, 0)
            x_step(4, 1)

    def one_block(b, carry):
        total = jnp.zeros((BR, COLS), jnp.float32)
        for k in range(2):
            total += jnp.dot(
                xg[b * 2 + k],
                wz[2 * k : 2 * k + 2].reshape(KB, COLS),
                preferred_element_type=jnp.float32,
            )
        acc[b] = total
        return carry

    lax.fori_loop(0, 4, one_block, 0)

    def rows_for(kx, kc):
        at = pl.multiple_of((kx * 2 + kc) * 24, 8)
        return acc[:, pl.ds(at, 24), :].reshape(RT, COLS)

    oc = 1 - c
    order = (2, 1, 3, 0)

    def d_copy(d):
        return remote(dsend.at[d], drecv.at[d], d2s.at[d], d2r.at[d], {"c": oc})

    for d in order:
        dsend[d] = rows_for(add(x, d, 4), oc).astype(jnp.bfloat16)
        d_copy(d).start()

    def r_copy(d):
        k = add(x, d, 4)
        return remote(rsend.at[d], rrecv.at[x], rss.at[d], rrs.at[x], {"x": k})

    for d in order:
        d_copy(d).wait_recv()
        total = rows_for(add(x, d, 4), c) + drecv[d].astype(jnp.float32)
        if d:
            rsend[d] = total.astype(jnp.bfloat16)
            r_copy(d).start()
        else:
            fin[pl.ds(0, RT), :] = total
    fin[pl.ds(RT, 8), :] = jnp.zeros((8, COLS), jnp.float32)
    for d in (1, 3, 2):
        k = add(x, d, 4)
        remote(rrecv.at[k], rrecv.at[k], rss.at[d], rrs.at[k], {"x": k}).wait_recv()
        fin[pl.ds(0, RT), :] += rrecv[k].astype(jnp.float32)

    def y_copy(d):
        k = add(y, d, 8)
        return remote(ysend.at[k], yrecv.at[y], yss.at[d], yrs.at[y], at_y(k))

    for k in range(8):
        ysend[k] = fin[pl.ds(OWN * k, 16), :].astype(jnp.bfloat16)
    for d in (4, 3, 5, 2, 6, 1, 7):
        y_copy(d).start()
    out_ref[y] = ysend[y]
    for d in range(1, 16):
        k = add(tp, d, 16)
        remote(strecv.at[k], strecv.at[k], sts.at[d], strs.at[k], at_tp(k)).wait_recv()
    sto_ref[...] = strecv[...]
    for d in range(1, 8):
        k = add(y, d, 8)
        remote(yrecv.at[k], yrecv.at[k], yss.at[d], yrs.at[k], at_y(k)).wait_recv()
        out_ref[k] = yrecv[k]

    for d in range(1, 8):
        a1_copy(d).wait_send()
        y_copy(d).wait_send()
    for d in range(1, 16):
        st_copy(d).wait_send()
    for d in range(1, 4):
        a2_copy(d).wait_send()
        r_copy(d).wait_send()

    @pl.when(zb != c)
    def _():
        a2_copy(0).wait_send()

    for d in range(4):
        d_copy(d).wait_send()
    for s in range(1, 5):
        for h in range(2):
            for way in range(2):
                if goes(s, h, way):
                    x_copy(s, h, way).wait_send()
                    mine, copy = w_copy(s, h, way)

                    @pl.when(mine)
                    def _(copy=copy):
                        copy.wait_send()


def project(x, w, st):
    vm = pltpu.VMEM
    dma = pltpu.SemaphoreType.DMA
    bf = jnp.bfloat16
    return pl.pallas_call(
        project_kernel,
        out_shape=(
            jax.ShapeDtypeStruct((8, 16, COLS), bf),
            jax.ShapeDtypeStruct((16, 8, 128), jnp.float32),
        ),
        in_specs=[pl.BlockSpec(memory_space=vm)] * 3,
        out_specs=(pl.BlockSpec(memory_space=vm),) * 2,
        scratch_shapes=[
            vm((8, BR, KB), bf),
            vm((8, 16, COLS), bf),
            vm((4, 4, 2, 2, 16, COLS), bf),
            vm((4, BR, COLS), jnp.float32),
            vm((4, RT, COLS), bf),
            vm((4, RT, COLS), bf),
            vm((4, RT, COLS), bf),
            vm((4, RT, COLS), bf),
            vm((RT + 8, COLS), jnp.float32),
            vm((8, 16, COLS), bf),
            vm((8, 16, COLS), bf),
            vm((16, 8, 128), jnp.float32),
            dma((2, 4, 2)), dma((2, 4, 2)),
            dma((8,)), dma((8,)),
            dma((4,)), dma((8,)),
            dma((2, 4, 2)), dma((2, 4, 2)),
            dma((16,)), dma((16,)),
            dma((4,)), dma((4,)),
            dma((4,)), dma((4,)),
            dma((8,)), dma((8,)),
        ],
        compiler_params=pltpu.CompilerParams(collective_id=0, has_side_effects=True),
        name="project",
    )(x, w, st)


def attend_kernel(len_ref, table_ref, qkv_ref, st_ref, kp_ref, vp_ref, out_ref, kbuf, vbuf, ksem, vsem):
    def page(r, m):
        at = table_ref[r, m]
        return (
            pltpu.make_async_copy(kp_ref.at[at], kbuf.at[r, :, m], ksem.at[r, m]),
            pltpu.make_async_copy(vp_ref.at[at], vbuf.at[r, :, m], vsem.at[r, m]),
        )

    for r in range(ROWS):
        for m in range(MOSTP):
            for copy in page(r, m):
                copy.start()

    rows16 = lax.broadcasted_iota(jnp.int32, (16, 128), 0)
    lanes16 = lax.broadcasted_iota(jnp.int32, (16, 128), 1)
    squares = jnp.sum(st_ref[:, 4, :], axis=0, keepdims=True)
    power = jnp.sum(
        jnp.where(rows16 == lanes16, jnp.broadcast_to(squares, (16, 128)), 0.0),
        axis=1,
        keepdims=True,
    )
    inv = lax.rsqrt(power * (1.0 / D) + EPS)
    keep = rows16 < OWN
    low = lanes16 < HD // 2

    row_of = rows16 // STEPS
    length = jnp.where(row_of == 0, len_ref[0], jnp.where(row_of == 1, len_ref[1], len_ref[2]))
    position = (length + lax.rem(rows16, STEPS)).astype(jnp.float32)
    pair = lax.rem(lanes16, HD // 2).astype(jnp.float32)
    freq = jnp.power(THETA, -(pair * 2.0 / HD))
    angle = position * freq
    cos, sin = jnp.cos(angle), jnp.sin(angle)
    sin = jnp.where(low, -sin, sin)

    def made(total, bias):
        value = (total * inv + bias).astype(jnp.bfloat16).astype(jnp.float32)
        return jnp.where(keep, value, 0.0)

    def rotated(value):
        return (value * cos + pltpu.roll(value, HD // 2, 1) * sin).astype(jnp.bfloat16)

    sel_row = lax.broadcasted_iota(jnp.int32, (32, 128), 0)
    sel_col = lax.broadcasted_iota(jnp.int32, (32, 128), 1)
    new_row = lax.broadcasted_iota(jnp.int32, (32, 16), 0)
    new_col = lax.broadcasted_iota(jnp.int32, (32, 16), 1)
    spot = lax.broadcasted_iota(jnp.int32, (32, MOSTP * PAGE), 1)
    scale = 1.0 / HD**0.5

    q_all, k_all, v_all = [], [], []
    for kh in range(KVH):
        heads = []
        for g in range(GROUP):
            h = kh * GROUP + g
            total = qkv_ref[h // 4, :, (h % 4) * HD : (h % 4 + 1) * HD].astype(jnp.float32)
            heads.append(rotated(made(total, st_ref[h // 2, h % 2 : h % 2 + 1, :])))
        q_all.append(jnp.concatenate(heads, axis=0))
        t0 = qkv_ref[2 * kh, :, 4 * HD : 5 * HD].astype(jnp.float32)
        t1 = qkv_ref[2 * kh + 1, :, 4 * HD : 5 * HD].astype(jnp.float32)
        k_bias = sum(st_ref[4 * kh + i, 2:3, :] for i in range(4))
        v_bias = sum(st_ref[4 * kh + i, 3:4, :] for i in range(4))
        k_sum = jnp.where(low, t0, pltpu.roll(t1, HD // 2, 1))
        v_sum = jnp.where(low, pltpu.roll(t0, HD // 2, 1), t1)
        k_all.append(rotated(made(k_sum, k_bias)))
        v_all.append(made(v_sum, v_bias).astype(jnp.bfloat16))

    contract = (((1,), (1,)), ((), ()))
    for r in range(ROWS):
        for m in range(MOSTP):
            for copy in page(r, m):
                copy.wait()
        want = (sel_row % GROUP) * 16 + r * STEPS + sel_row // GROUP
        pick = jnp.where(sel_col == want, 1.0, 0.0).astype(jnp.bfloat16)
        live = spot < len_ref[r]
        fresh_live = (new_col // STEPS == r) & (lax.rem(new_col, STEPS) <= new_row // GROUP)
        for kh in range(KVH):
            q = jnp.dot(pick, q_all[kh], preferred_element_type=jnp.float32).astype(jnp.bfloat16)
            keys = kbuf[r, kh].reshape(MOSTP * PAGE, HD)
            vals = vbuf[r, kh].reshape(MOSTP * PAGE, HD)
            cache = lax.dot_general(q, keys, contract, preferred_element_type=jnp.float32) * scale
            cache = jnp.where(live, cache, -1e30)
            fresh = (
                lax.dot_general(q, k_all[kh], contract, preferred_element_type=jnp.float32) * scale
            )
            fresh = jnp.where(fresh_live, fresh, -1e30)
            top = jnp.maximum(
                jnp.max(cache, axis=1, keepdims=True), jnp.max(fresh, axis=1, keepdims=True)
            )
            e_cache = jnp.where(live, jnp.exp(cache - top), 0.0)
            e_fresh = jnp.where(fresh_live, jnp.exp(fresh - top), 0.0)
            total = jnp.sum(e_cache, axis=1, keepdims=True) + jnp.sum(e_fresh, axis=1, keepdims=True)
            share = 1.0 / total
            w_cache = (e_cache * share).astype(jnp.bfloat16)
            w_fresh = (e_fresh * share).astype(jnp.bfloat16)
            out = jnp.dot(w_cache, vals, preferred_element_type=jnp.float32)
            out += jnp.dot(w_fresh, v_all[kh], preferred_element_type=jnp.float32)
            for t in range(STEPS):
                out_ref[r, t, kh * GROUP : (kh + 1) * GROUP, :] = out[t * GROUP : (t + 1) * GROUP, :]


def attend(lengths, table, qkv, st, key_pages, value_pages):
    vm = pltpu.VMEM
    return pl.pallas_call(
        attend_kernel,
        out_shape=jax.ShapeDtypeStruct((ROWS, STEPS, HQ, HD), jnp.float32),
        in_specs=[pl.BlockSpec(memory_space=pltpu.SMEM)] * 2
        + [pl.BlockSpec(memory_space=vm)] * 2
        + [pl.BlockSpec(memory_space=pl.ANY)] * 2,
        out_specs=pl.BlockSpec(memory_space=vm),
        scratch_shapes=[
            vm((ROWS, KVH, MOSTP, PAGE, HD), jnp.bfloat16),
            vm((ROWS, KVH, MOSTP, PAGE, HD), jnp.bfloat16),
            pltpu.SemaphoreType.DMA((ROWS, MOSTP)),
            pltpu.SemaphoreType.DMA((ROWS, MOSTP)),
        ],
        name="attend",
    )(lengths, table, qkv, st, key_pages, value_pages)


def on_device(
    hidden,
    norm_gain,
    w_query,
    w_key,
    w_value,
    bias_query,
    bias_key,
    bias_value,
    key_pages,
    value_pages,
    kv_lengths,
    page_table,
):
    tp = lax.axis_index(TP)
    block = lax.axis_index(REPLICA) * 16 + tp
    gain = lax.dynamic_slice(norm_gain, (block * 16,), (16,))
    weights = jnp.concatenate(
        [w_query.reshape(16, 8, 512), w_key.reshape(16, 8, 64), w_value.reshape(16, 8, 64)], axis=2
    )
    weights = (weights * gain[:, None, None]).astype(jnp.bfloat16).transpose(1, 0, 2)
    rows = hidden.reshape(4, 2, 2, OWN, KB).transpose(0, 2, 1, 3, 4).reshape(BR, KB)
    wide = hidden.astype(jnp.float32)
    squares = jnp.sum(wide * wide, axis=2).reshape(16, 1, OWN)
    lane = jnp.arange(128)
    place = (lane // 32) == lax.rem(tp, 4)
    k_bias = jnp.where(place, jnp.tile(bias_key, 4), 0.0)
    v_bias = jnp.where(place, jnp.tile(bias_value, 4), 0.0)
    shared = jnp.concatenate([bias_query.reshape(2, 128), k_bias[None], v_bias[None]], axis=0)
    stats = jnp.concatenate(
        [
            jnp.broadcast_to(shared[None], (16, 4, 128)),
            jnp.pad(squares, ((0, 0), (0, 3), (0, 128 - OWN))),
        ],
        axis=1,
    )
    stats = jnp.pad(stats, ((0, 0), (0, 8 - stats.shape[1]), (0, 0)))
    qkv, stats = project(rows, weights, stats)
    out = attend(kv_lengths, page_table, qkv, stats, key_pages, value_pages)
    return out.astype(jnp.bfloat16).reshape(ROWS, STEPS, HQ * HD)


def solution(mesh):
    split = Mesh(mesh.devices.reshape(4, 8, 4, 2, 2), AXES)
    both = REPLICA + TP
    in_specs = (
        P(REPLICA, None, TP),
        P(),
        P(both, None),
        P(both, None),
        P(both, None),
        P(TP),
        P(TP),
        P(TP),
        P(both, None, None, None),
        P(both, None, None, None),
        P(both),
        P(both, None),
    )
    return jax.shard_map(
        on_device, mesh=split, in_specs=in_specs, out_specs=P(both, None, None), check_vma=False
    )
```

```python
import functools

import jax
import jax.numpy as jnp
from jax import lax
from jax.experimental import pallas as pl
from jax.experimental.pallas import tpu as pltpu
from jax.sharding import Mesh
from jax.sharding import PartitionSpec as P

HD = 128
HQ = 32
KVH = 4
GROUP = HQ // KVH
PAGE = 128
MOSTP = 8
STEPS = 4
ROWS = 3
OWN = ROWS * STEPS
D = 8192
EPS = 1e-06
THETA = 1000000.0
MESH = pl.DeviceIdType.MESH
AXES = ("yh", "z", "x", "yl", "c")
TP = ("x", "yl", "c")
REPLICA = ("yh", "z")
COLS = 640
KB = 512
BR = 192
RT = 96


def remote(src, dst, send, recv, where):
    return pltpu.make_async_remote_copy(
        src_ref=src, dst_ref=dst, send_sem=send, recv_sem=recv, device_id=where, device_id_type=MESH
    )


def column_of(row, shape):
    rows = lax.broadcasted_iota(jnp.int32, shape, 0)
    lanes = lax.broadcasted_iota(jnp.int32, shape, 1)
    return jnp.sum(
        jnp.where(rows == lanes, jnp.broadcast_to(row, shape), 0.0), axis=1, keepdims=True
    )


def prepare(
    block, h_ref, gain_ref, wq_ref, wk_ref, wv_ref, bq_ref, bk_ref, bv_ref, w_ref, st_ref
):
    row = gain_ref[pl.ds(block // 8, 1), :]
    rows = lax.broadcasted_iota(jnp.int32, (16, 128), 0)
    lanes = lax.broadcasted_iota(jnp.int32, (16, 128), 1)
    low = lanes < HD // 2
    gain = jnp.sum(
        jnp.where(lanes == rows + lax.rem(block, 8) * 16, jnp.broadcast_to(row, (16, 128)), 0.0),
        axis=1,
        keepdims=True,
    )
    for k in range(8):
        w_ref[k, :, 0:512] = (wq_ref[:, 512 * k : 512 * k + 512] * gain).astype(jnp.bfloat16)
        tiles = slice(HD * (k // 2), HD * (k // 2) + HD)
        tk, tv = wk_ref[:, tiles] * gain, wv_ref[:, tiles] * gain
        if k % 2 == 0:
            both = jnp.where(low, tk, pltpu.roll(tv, HD // 2, 1))
        else:
            both = jnp.where(low, pltpu.roll(tk, HD // 2, 1), tv)
        w_ref[k, :, 512:640] = both.astype(jnp.bfloat16)

    wide = h_ref[...].astype(jnp.float32)
    squares = jnp.sum(wide * wide, axis=1, keepdims=True)
    of_row = lax.broadcasted_iota(jnp.int32, (BR, 128), 0)
    of_lane = lax.broadcasted_iota(jnp.int32, (BR, 128), 1)
    spread = jnp.where(lax.rem(of_row, OWN) == of_lane, squares, 0.0)
    group = lax.broadcasted_iota(jnp.int32, (16, BR), 0)
    member = lax.broadcasted_iota(jnp.int32, (16, BR), 1)
    owner = jnp.where(member // OWN == group, 1.0, 0.0)
    per_owner = jnp.dot(
        owner, spread, preferred_element_type=jnp.float32, precision=lax.Precision.HIGHEST
    )
    for k in range(16):
        st_ref[k, 0:2, :] = bq_ref[...]
        st_ref[k, 2:3, 0:32] = bk_ref[...]
        st_ref[k, 3:4, 0:32] = bv_ref[...]
        st_ref[k, 4:5, :] = per_owner[k : k + 1, :]


def turns(len_ref, rope):
    rows = lax.broadcasted_iota(jnp.int32, (16, 128), 0)
    lanes = lax.broadcasted_iota(jnp.int32, (16, 128), 1)
    row_of = rows // STEPS
    length = jnp.where(row_of == 0, len_ref[0], jnp.where(row_of == 1, len_ref[1], len_ref[2]))
    position = (length + lax.rem(rows, STEPS)).astype(jnp.float32)
    pair = lax.rem(lanes, HD // 2).astype(jnp.float32)
    freq = jnp.power(THETA, -(pair * 2.0 / HD))
    angle = position * freq
    rope[0] = jnp.cos(angle)
    sin = jnp.sin(angle)
    rope[1] = jnp.where(lanes < HD // 2, -sin, sin)


def row_scale(strecv):
    squares = jnp.sum(strecv[:, 4, :], axis=0, keepdims=True)
    return lax.rsqrt(column_of(squares, (16, 128)) * (1.0 / D) + EPS)


def attend(kh, inv, len_ref, table_ref, qkv, st, rope, kpool, vpool, out_ref):
    rows = lax.broadcasted_iota(jnp.int32, (16, 128), 0)
    lanes = lax.broadcasted_iota(jnp.int32, (16, 128), 1)
    keep = rows < OWN
    low = lanes < HD // 2
    cos, sin = rope[0], rope[1]

    def made(total, bias):
        value = (total * inv + bias).astype(jnp.bfloat16).astype(jnp.float32)
        return jnp.where(keep, value, 0.0)

    def rotated(value):
        return (value * cos + pltpu.roll(value, HD // 2, 1) * sin).astype(jnp.bfloat16)

    def small_bias(at):
        lane = lax.broadcasted_iota(jnp.int32, (1, 128), 1)
        out = jnp.zeros((1, 128), jnp.float32)
        for i in range(4):
            piece = st[4 * kh + i, at : at + 1, :]
            if i:
                piece = pltpu.roll(piece, 32 * i, 1)
            out = jnp.where(lane // 32 == i, piece, out)
        return out

    heads = []
    for g in range(GROUP):
        i, a = g // 4, g % 4
        total = qkv[2 * kh + i, :, a * HD : (a + 1) * HD].astype(jnp.float32)
        bias = st[2 * (2 * kh + i) + a // 2, a % 2 : a % 2 + 1, :]
        heads.append(rotated(made(total, bias)))
    q_all = jnp.concatenate(heads, axis=0)
    t0 = qkv[2 * kh, :, 4 * HD : 5 * HD].astype(jnp.float32)
    t1 = qkv[2 * kh + 1, :, 4 * HD : 5 * HD].astype(jnp.float32)
    k_new = rotated(made(jnp.where(low, t0, pltpu.roll(t1, HD // 2, 1)), small_bias(2)))
    v_new = made(jnp.where(low, pltpu.roll(t0, HD // 2, 1), t1), small_bias(3))
    v_new = v_new.astype(jnp.bfloat16)

    sel_row = lax.broadcasted_iota(jnp.int32, (32, 128), 0)
    sel_col = lax.broadcasted_iota(jnp.int32, (32, 128), 1)
    new_row = lax.broadcasted_iota(jnp.int32, (32, 16), 0)
    new_col = lax.broadcasted_iota(jnp.int32, (32, 16), 1)
    spot = lax.broadcasted_iota(jnp.int32, (32, MOSTP * PAGE), 1)
    scale = 1.0 / HD**0.5
    contract = (((1,), (1,)), ((), ()))
    for r in range(ROWS):
        want = (sel_row // STEPS) * 16 + r * STEPS + lax.rem(sel_row, STEPS)
        pick = jnp.where(sel_col == want, 1.0, 0.0).astype(jnp.bfloat16)
        live = spot < len_ref[r]
        fresh_live = (new_col // STEPS == r) & (lax.rem(new_col, STEPS) <= lax.rem(new_row, STEPS))
        q = jnp.dot(pick, q_all, preferred_element_type=jnp.float32).astype(jnp.bfloat16)
        keys = jnp.concatenate([kpool[table_ref[r, m], kh] for m in range(MOSTP)], axis=0)
        vals = jnp.concatenate([vpool[table_ref[r, m], kh] for m in range(MOSTP)], axis=0)
        cache = lax.dot_general(q, keys, contract, preferred_element_type=jnp.float32) * scale
        cache = jnp.where(live, cache, -1e30)
        fresh = lax.dot_general(q, k_new, contract, preferred_element_type=jnp.float32) * scale
        fresh = jnp.where(fresh_live, fresh, -1e30)
        top = jnp.maximum(
            jnp.max(cache, axis=1, keepdims=True), jnp.max(fresh, axis=1, keepdims=True)
        )
        e_cache = jnp.where(live, jnp.exp(cache - top), 0.0)
        e_fresh = jnp.where(fresh_live, jnp.exp(fresh - top), 0.0)
        total = jnp.sum(e_cache, axis=1, keepdims=True) + jnp.sum(e_fresh, axis=1, keepdims=True)
        share = 1.0 / total
        w_cache = (e_cache * share).astype(jnp.bfloat16)
        w_fresh = (e_fresh * share).astype(jnp.bfloat16)
        out = jnp.dot(w_cache, vals, preferred_element_type=jnp.float32)
        out += jnp.dot(w_fresh, v_new, preferred_element_type=jnp.float32)
        for g in range(GROUP):
            at = pl.ds(pl.multiple_of(kh * GROUP * HD + g * HD, HD), HD)
            out_ref[r, :, at] = out[g * STEPS : (g + 1) * STEPS, :].astype(jnp.bfloat16)


def step_kernel(
    len_ref, table_ref, h_ref, gain_ref, wq_ref, wk_ref, wv_ref, bq_ref, bk_ref, bv_ref, kp_ref, vp_ref,
    out_ref,
    w_ref, st_ref, rope, kpool, vpool,
    xg, a1, wz, acc, dsend, drecv, rsend, rrecv, fin, ysend, yrecv, strecv,
    pools, xs, xr, a1s, a1r, a2s, a2r, ws, wr, sts, strs, d2s, d2r, rss, rrs, yss, yrs,
):
    yh, z, x, yl, c = (lax.axis_index(a) for a in AXES)
    y = yh * 2 + yl
    tp = x * 4 + yl * 2 + c
    zb = lax.rem(z // 2, 2)

    def at_y(k):
        return {"yh": k // 2, "yl": lax.rem(k, 2)}

    def at_tp(k):
        return {"x": k // 4, "yl": lax.rem(k // 2, 2), "c": lax.rem(k, 2)}

    def add(a, k, n):
        return lax.rem(a + (k + n) % n, n)

    pool_copies = (
        pltpu.make_async_copy(kp_ref, kpool, pools.at[0]),
        pltpu.make_async_copy(vp_ref, vpool, pools.at[1]),
    )
    for copy in pool_copies:
        copy.start()

    barrier = pltpu.get_barrier_semaphore()
    for d in range(1, 16):
        pl.semaphore_signal(barrier, inc=1, device_id=at_tp(add(tp, d, 16)), device_id_type=MESH)
    for d in range(1, 4):
        for k in range(4):
            pl.semaphore_signal(
                barrier,
                inc=1,
                device_id={"yh": add(yh, d, 4), "yl": k // 2, "c": k % 2},
                device_id_type=MESH,
            )
    for d in (1, -1):
        pl.semaphore_signal(barrier, inc=1, device_id={"z": add(z, d, 8)}, device_id_type=MESH)

    prepare(
        (yh * 8 + z) * 16 + tp, h_ref, gain_ref, wq_ref, wk_ref, wv_ref, bq_ref, bk_ref, bv_ref,
        w_ref, st_ref,
    )
    pl.semaphore_wait(barrier, 29)

    y_next = (at_y(add(y, 1, 8)), at_y(add(y, -1, 8)))
    z_next = ({"z": add(z, 1, 8)}, {"z": add(z, -1, 8)})

    def x_copy(s, h, way):
        o = add(y, -(s - 1) if way == 0 else s - 1, 8)
        rows = pl.ds(RT * h, RT)
        src = h_ref.at[rows] if s == 1 else xg.at[o, rows]
        return remote(
            src, xg.at[o, rows], xs.at[way, s - 1, h], xr.at[way, s - 1, h], y_next[way]
        )

    def x_wait(s, h, way):
        o = add(y, -s if way == 0 else s, 8)
        dst = xg.at[o, pl.ds(RT * h, RT)]
        remote(dst, dst, xs.at[way, s - 1, h], xr.at[way, s - 1, h], y_next[way]).wait_recv()

    def goes(s, h, way):
        return s <= 3 or (s == 4 and h == way)

    def origin_w(s, way):
        o = add(z, -s if way == 0 else s, 8)
        return o, lax.rem(o // 2, 2) == c, (o // 4) * 2 + lax.rem(o, 2)

    def w_copy(s, h, way):
        _, mine, j = origin_w(s - 1, way)
        part = wz.at[j, pl.ds(2 * h, 2)]
        return mine, remote(
            part, part, ws.at[way, s - 1, h], wr.at[way, s - 1, h], z_next[way]
        )

    def w_send(s, h, way):
        mine, copy = w_copy(s, h, way)

        @pl.when(mine)
        def _():
            copy.start()

    def w_step(s, h, way):
        _, mine, j = origin_w(s, way)
        part = wz.at[j, pl.ds(2 * h, 2)]

        @pl.when(mine)
        def _():
            remote(
                part, part, ws.at[way, s - 1, h], wr.at[way, s - 1, h], z_next[way]
            ).wait_recv()
            if goes(s + 1, h, way):
                w_copy(s + 1, h, way)[1].start()

    def x_step(s, h):
        for way in range(2):
            if goes(s, h, way):
                x_wait(s, h, way)
                if goes(s + 1, h, way):
                    x_copy(s + 1, h, way).start()

    def a1_copy(d):
        k = add(y, d, 8)
        return remote(w_ref.at[k], a1.at[y], a1s.at[d], a1r.at[y], at_y(k))

    for d in (4, 3, 5, 2, 6, 1, 7):
        a1_copy(d).start()
    for h in range(2):
        for way in range(2):
            x_copy(1, h, way).start()

    def st_copy(d):
        k = add(tp, d, 16)
        return remote(st_ref.at[k], strecv.at[tp], sts.at[d], strs.at[tp], at_tp(k))

    for d in range(1, 16):
        st_copy(d).start()
    a1[y] = w_ref[y]
    xg[y] = h_ref[...]
    strecv[tp] = st_ref[tp]
    turns(len_ref, rope)

    for d in range(1, 8):
        k = add(y, d, 8)
        remote(a1.at[k], a1.at[k], a1s.at[d], a1r.at[k], at_y(k)).wait_recv()

    own_j = (z // 4) * 2 + lax.rem(z, 2)

    def a2_copy(d):
        k = add(x, d, 4)
        return remote(
            a1.at[pl.ds(2 * k, 2)],
            wz.at[own_j, x, :, c],
            a2s.at[d],
            a2r.at[x * 2 + c],
            {"x": k, "c": zb},
        )

    for d in (2, 1, 3):
        a2_copy(d).start()

    @pl.when(zb != c)
    def _():
        a2_copy(0).start()

    @pl.when(zb == c)
    def _():
        wz[own_j, x, :, c] = a1[pl.ds(2 * x, 2)]

    x_step(1, 0)
    x_step(1, 1)

    @pl.when(zb == c)
    def _():
        for d in range(8):
            k = add(x * 2 + c, d, 8)
            kx, kc = k // 2, lax.rem(k, 2)
            dst = wz.at[own_j, kx, :, kc]
            if d > 0:
                remote(dst, dst, a2s.at[0], a2r.at[k], {"x": kx, "c": kc}).wait_recv()

    for h in range(2):
        for way in range(2):
            w_send(1, h, way)
    x_step(2, 0)
    x_step(2, 1)
    for s in range(1, 5):
        for h in range(2):
            for way in range(2):
                if goes(s, h, way):
                    w_step(s, h, way)
        if s == 1:
            x_step(3, 0)
            x_step(3, 1)
        if s == 2:
            x_step(4, 0)
            x_step(4, 1)

    def one_block(b, carry):
        total = jnp.zeros((BR, COLS), jnp.float32)
        for k in range(2):
            total += jnp.dot(
                xg[b * 2 + k],
                wz[2 * k : 2 * k + 2].reshape(KB, COLS),
                preferred_element_type=jnp.float32,
            )
        acc[b] = total
        return carry

    lax.fori_loop(0, 4, one_block, 0)

    def rows_for(kx, kc):
        at = pl.multiple_of((kx * 2 + kc) * 24, 8)
        return acc[:, pl.ds(at, 24), :].reshape(RT, COLS)

    oc = 1 - c
    order = (2, 1, 3, 0)

    def d_copy(d):
        return remote(dsend.at[d], drecv.at[d], d2s.at[d], d2r.at[d], {"c": oc})

    for d in order:
        dsend[d] = rows_for(add(x, d, 4), oc).astype(jnp.bfloat16)
        d_copy(d).start()

    def r_copy(d):
        k = add(x, d, 4)
        return remote(rsend.at[d], rrecv.at[x], rss.at[d], rrs.at[x], {"x": k})

    for d in order:
        d_copy(d).wait_recv()
        total = rows_for(add(x, d, 4), c) + drecv[d].astype(jnp.float32)
        if d:
            rsend[d] = total.astype(jnp.bfloat16)
            r_copy(d).start()
        else:
            fin[pl.ds(0, RT), :] = total
    fin[pl.ds(RT, 8), :] = jnp.zeros((8, COLS), jnp.float32)
    for d in (1, 3, 2):
        k = add(x, d, 4)
        remote(rrecv.at[k], rrecv.at[k], rss.at[d], rrs.at[k], {"x": k}).wait_recv()
        fin[pl.ds(0, RT), :] += rrecv[k].astype(jnp.float32)

    def y_copy(d, dc):
        k = add(yh, d, 4)
        kc = lax.rem(c + dc, 2)
        return remote(
            ysend.at[k, kc],
            yrecv.at[y],
            yss.at[d, dc],
            yrs.at[y],
            {"yh": k, "yl": c, "c": kc},
        )

    def y_each(act):
        for d in (0, 1, 3, 2):
            for dc in range(2):
                if d == 0 and dc == 0:

                    @pl.when(yl != c)
                    def _():
                        act(y_copy(0, 0))
                else:
                    act(y_copy(d, dc))

    for k in range(4):
        for kc in range(2):
            ysend[k, kc] = fin[pl.ds(24 * k + OWN * kc, 16), :].astype(jnp.bfloat16)
    y_each(lambda copy: copy.start())

    @pl.when(yl == c)
    def _():
        yrecv[y] = ysend[yh, c]

    for d in range(1, 16):
        k = add(tp, d, 16)
        remote(strecv.at[k], strecv.at[k], sts.at[d], strs.at[k], at_tp(k)).wait_recv()
    for copy in pool_copies:
        copy.wait()

    inv = row_scale(strecv)

    def one_group(d, carry):
        kh = lax.rem(yh + jnp.where(d == 2, 3, jnp.where(d == 3, 2, d)), 4)
        for i in range(2):
            k = kh * 2 + i

            @pl.when((k != y) | (yl != c))
            def _(k=k):
                remote(
                    yrecv.at[k], yrecv.at[k], yss.at[1, 0], yrs.at[k], {"yh": add(yh, 1, 4)}
                ).wait_recv()

        attend(kh, inv, len_ref, table_ref, yrecv, strecv, rope, kpool, vpool, out_ref)
        return carry

    lax.fori_loop(0, 4, one_group, 0)

    for d in range(1, 8):
        a1_copy(d).wait_send()
    y_each(lambda copy: copy.wait_send())
    for d in range(1, 16):
        st_copy(d).wait_send()
    for d in range(1, 4):
        a2_copy(d).wait_send()
        r_copy(d).wait_send()

    @pl.when(zb != c)
    def _():
        a2_copy(0).wait_send()

    for d in range(4):
        d_copy(d).wait_send()
    for s in range(1, 5):
        for h in range(2):
            for way in range(2):
                if goes(s, h, way):
                    x_copy(s, h, way).wait_send()
                    mine, copy = w_copy(s, h, way)

                    @pl.when(mine)
                    def _(copy=copy):
                        copy.wait_send()


def on_device(
    hidden,
    norm_gain,
    w_query,
    w_key,
    w_value,
    bias_query,
    bias_key,
    bias_value,
    key_pages,
    value_pages,
    kv_lengths,
    page_table,
):
    vm = pltpu.VMEM
    dma = pltpu.SemaphoreType.DMA
    bf = jnp.bfloat16
    f32 = jnp.float32
    return pl.pallas_call(
        step_kernel,
        out_shape=jax.ShapeDtypeStruct((ROWS, STEPS, HQ * HD), bf),
        in_specs=[pl.BlockSpec(memory_space=pltpu.SMEM)] * 2
        + [pl.BlockSpec(memory_space=vm)] * 8
        + [pl.BlockSpec(memory_space=pl.ANY)] * 2,
        out_specs=pl.BlockSpec(memory_space=vm),
        scratch_shapes=[
            vm((8, 16, COLS), bf),
            vm((16, 8, 128), f32),
            vm((2, 16, 128), f32),
            vm((16, KVH, PAGE, HD), bf),
            vm((16, KVH, PAGE, HD), bf),
            vm((8, BR, KB), bf),
            vm((8, 16, COLS), bf),
            vm((4, 4, 2, 2, 16, COLS), bf),
            vm((4, BR, COLS), f32),
            vm((4, RT, COLS), bf),
            vm((4, RT, COLS), bf),
            vm((4, RT, COLS), bf),
            vm((4, RT, COLS), bf),
            vm((RT + 8, COLS), f32),
            vm((4, 2, 16, COLS), bf),
            vm((8, 16, COLS), bf),
            vm((16, 8, 128), f32),
            dma((2,)),
            dma((2, 4, 2)), dma((2, 4, 2)),
            dma((8,)), dma((8,)),
            dma((4,)), dma((8,)),
            dma((2, 4, 2)), dma((2, 4, 2)),
            dma((16,)), dma((16,)),
            dma((4,)), dma((4,)),
            dma((4,)), dma((4,)),
            dma((4, 2)), dma((8,)),
        ],
        compiler_params=pltpu.CompilerParams(collective_id=0, has_side_effects=True),
        name="step",
    )(
        kv_lengths,
        page_table,
        hidden.reshape(BR, KB),
        norm_gain.reshape(D // 128, 128),
        w_query,
        w_key,
        w_value,
        bias_query.reshape(2, 128),
        bias_key.reshape(1, 32),
        bias_value.reshape(1, 32),
        key_pages,
        value_pages,
    )


def solution(mesh):
    split = Mesh(mesh.devices.reshape(4, 8, 4, 2, 2), AXES)
    both = REPLICA + TP
    in_specs = (
        P(REPLICA, None, TP),
        P(),
        P(both, None),
        P(both, None),
        P(both, None),
        P(TP),
        P(TP),
        P(TP),
        P(both, None, None, None),
        P(both, None, None, None),
        P(both),
        P(both, None),
    )
    return jax.shard_map(
        on_device, mesh=split, in_specs=in_specs, out_specs=P(both, None, None), check_vma=False
    )
```

```python
import functools

import jax
import jax.numpy as jnp
from jax import lax
from jax.experimental import pallas as pl
from jax.experimental.pallas import tpu as pltpu
from jax.sharding import Mesh
from jax.sharding import PartitionSpec as P

HD = 128
HQ = 32
KVH = 4
GROUP = HQ // KVH
PAGE = 128
MOSTP = 8
STEPS = 4
ROWS = 3
OWN = ROWS * STEPS
D = 8192
EPS = 1e-06
THETA = 1000000.0
MESH = pl.DeviceIdType.MESH
AXES = ("yh", "z", "x", "yl", "c")
TP = ("x", "yl", "c")
REPLICA = ("yh", "z")
COLS = 640
KB = 512
BR = 192
RT = 96


def remote(src, dst, send, recv, where):
    return pltpu.make_async_remote_copy(
        src_ref=src, dst_ref=dst, send_sem=send, recv_sem=recv, device_id=where, device_id_type=MESH
    )


def column_of(row, shape):
    rows = lax.broadcasted_iota(jnp.int32, shape, 0)
    lanes = lax.broadcasted_iota(jnp.int32, shape, 1)
    return jnp.sum(
        jnp.where(rows == lanes, jnp.broadcast_to(row, shape), 0.0), axis=1, keepdims=True
    )


def cast_weights(block, gain_ref, wq_ref, wk_ref, wv_ref, w_ref):
    row = gain_ref[pl.ds(block // 8, 1), :]
    rows = lax.broadcasted_iota(jnp.int32, (16, 128), 0)
    lanes = lax.broadcasted_iota(jnp.int32, (16, 128), 1)
    low = lanes < HD // 2
    gain = jnp.sum(
        jnp.where(lanes == rows + lax.rem(block, 8) * 16, jnp.broadcast_to(row, (16, 128)), 0.0),
        axis=1,
        keepdims=True,
    )
    for k in range(8):
        w_ref[k, :, 0:512] = (wq_ref[:, 512 * k : 512 * k + 512] * gain).astype(jnp.bfloat16)
        tiles = slice(HD * (k // 2), HD * (k // 2) + HD)
        tk, tv = wk_ref[:, tiles] * gain, wv_ref[:, tiles] * gain
        if k % 2 == 0:
            both = jnp.where(low, tk, pltpu.roll(tv, HD // 2, 1))
        else:
            both = jnp.where(low, pltpu.roll(tk, HD // 2, 1), tv)
        w_ref[k, :, 512:640] = both.astype(jnp.bfloat16)


def fill_stats(h_ref, bq_ref, bk_ref, bv_ref, st_ref):
    wide = h_ref[...].astype(jnp.float32)
    squares = jnp.sum(wide * wide, axis=1, keepdims=True)
    of_row = lax.broadcasted_iota(jnp.int32, (BR, 128), 0)
    of_lane = lax.broadcasted_iota(jnp.int32, (BR, 128), 1)
    spread = jnp.where(lax.rem(of_row, OWN) == of_lane, squares, 0.0)
    group = lax.broadcasted_iota(jnp.int32, (16, BR), 0)
    member = lax.broadcasted_iota(jnp.int32, (16, BR), 1)
    owner = jnp.where(member // OWN == group, 1.0, 0.0)
    per_owner = jnp.dot(
        owner, spread, preferred_element_type=jnp.float32, precision=lax.Precision.HIGHEST
    )
    for k in range(16):
        st_ref[k, 0:2, :] = bq_ref[...]
        st_ref[k, 2:3, 0:32] = bk_ref[...]
        st_ref[k, 3:4, 0:32] = bv_ref[...]
        st_ref[k, 4:5, :] = per_owner[k : k + 1, :]


def turns(len_ref, rope):
    rows = lax.broadcasted_iota(jnp.int32, (16, 128), 0)
    lanes = lax.broadcasted_iota(jnp.int32, (16, 128), 1)
    row_of = rows // STEPS
    length = jnp.where(row_of == 0, len_ref[0], jnp.where(row_of == 1, len_ref[1], len_ref[2]))
    position = (length + lax.rem(rows, STEPS)).astype(jnp.float32)
    pair = lax.rem(lanes, HD // 2).astype(jnp.float32)
    freq = jnp.power(THETA, -(pair * 2.0 / HD))
    angle = position * freq
    rope[0] = jnp.cos(angle)
    sin = jnp.sin(angle)
    rope[1] = jnp.where(lanes < HD // 2, -sin, sin)


def row_scale(strecv):
    squares = jnp.sum(strecv[:, 4, :], axis=0, keepdims=True)
    return lax.rsqrt(column_of(squares, (16, 128)) * (1.0 / D) + EPS)


def attend(kh, inv, len_ref, table_ref, qkv, st, rope, kpool, vpool, out_ref):
    rows = lax.broadcasted_iota(jnp.int32, (16, 128), 0)
    lanes = lax.broadcasted_iota(jnp.int32, (16, 128), 1)
    keep = rows < OWN
    low = lanes < HD // 2
    cos, sin = rope[0], rope[1]

    def made(total, bias):
        value = (total * inv + bias).astype(jnp.bfloat16).astype(jnp.float32)
        return jnp.where(keep, value, 0.0)

    def rotated(value):
        return (value * cos + pltpu.roll(value, HD // 2, 1) * sin).astype(jnp.bfloat16)

    def small_bias(at):
        lane = lax.broadcasted_iota(jnp.int32, (1, 128), 1)
        out = jnp.zeros((1, 128), jnp.float32)
        for i in range(4):
            piece = st[4 * kh + i, at : at + 1, :]
            if i:
                piece = pltpu.roll(piece, 32 * i, 1)
            out = jnp.where(lane // 32 == i, piece, out)
        return out

    heads = []
    for g in range(GROUP):
        i, a = g // 4, g % 4
        total = qkv[2 * kh + i, :, a * HD : (a + 1) * HD].astype(jnp.float32)
        bias = st[2 * (2 * kh + i) + a // 2, a % 2 : a % 2 + 1, :]
        heads.append(rotated(made(total, bias)))
    q_all = jnp.concatenate(heads, axis=0)
    t0 = qkv[2 * kh, :, 4 * HD : 5 * HD].astype(jnp.float32)
    t1 = qkv[2 * kh + 1, :, 4 * HD : 5 * HD].astype(jnp.float32)
    k_new = rotated(made(jnp.where(low, t0, pltpu.roll(t1, HD // 2, 1)), small_bias(2)))
    v_new = made(jnp.where(low, pltpu.roll(t0, HD // 2, 1), t1), small_bias(3))
    v_new = v_new.astype(jnp.bfloat16)

    sel_row = lax.broadcasted_iota(jnp.int32, (32, 128), 0)
    sel_col = lax.broadcasted_iota(jnp.int32, (32, 128), 1)
    new_row = lax.broadcasted_iota(jnp.int32, (32, 16), 0)
    new_col = lax.broadcasted_iota(jnp.int32, (32, 16), 1)
    spot = lax.broadcasted_iota(jnp.int32, (32, MOSTP * PAGE), 1)
    scale = 1.0 / HD**0.5
    contract = (((1,), (1,)), ((), ()))
    for r in range(ROWS):
        want = (sel_row // STEPS) * 16 + r * STEPS + lax.rem(sel_row, STEPS)
        pick = jnp.where(sel_col == want, 1.0, 0.0).astype(jnp.bfloat16)
        live = spot < len_ref[r]
        fresh_live = (new_col // STEPS == r) & (lax.rem(new_col, STEPS) <= lax.rem(new_row, STEPS))
        q = jnp.dot(pick, q_all, preferred_element_type=jnp.float32).astype(jnp.bfloat16)
        keys = jnp.concatenate([kpool[table_ref[r, m], kh] for m in range(MOSTP)], axis=0)
        vals = jnp.concatenate([vpool[table_ref[r, m], kh] for m in range(MOSTP)], axis=0)
        cache = lax.dot_general(q, keys, contract, preferred_element_type=jnp.float32) * scale
        cache = jnp.where(live, cache, -1e30)
        fresh = lax.dot_general(q, k_new, contract, preferred_element_type=jnp.float32) * scale
        fresh = jnp.where(fresh_live, fresh, -1e30)
        top = jnp.maximum(
            jnp.max(cache, axis=1, keepdims=True), jnp.max(fresh, axis=1, keepdims=True)
        )
        e_cache = jnp.where(live, jnp.exp(cache - top), 0.0)
        e_fresh = jnp.where(fresh_live, jnp.exp(fresh - top), 0.0)
        total = jnp.sum(e_cache, axis=1, keepdims=True) + jnp.sum(e_fresh, axis=1, keepdims=True)
        share = 1.0 / total
        w_cache = (e_cache * share).astype(jnp.bfloat16)
        w_fresh = (e_fresh * share).astype(jnp.bfloat16)
        out = jnp.dot(w_cache, vals, preferred_element_type=jnp.float32)
        out += jnp.dot(w_fresh, v_new, preferred_element_type=jnp.float32)
        for g in range(GROUP):
            at = pl.ds(pl.multiple_of(kh * GROUP * HD + g * HD, HD), HD)
            out_ref[r, :, at] = out[g * STEPS : (g + 1) * STEPS, :]


def step_kernel(
    len_ref, table_ref, h_hbm, gain_hbm, wq_hbm, wk_hbm, wv_hbm, bq_hbm, bk_hbm, bv_hbm, kp_ref, vp_ref,
    out_ref,
    raw, gain_ref, wq_ref, wk_ref, wv_ref, bq_ref, bk_ref, bv_ref, h_ref,
    w_ref, st_ref, rope, kpool, vpool,
    xg, a1, wz, acc, dsend, drecv, rsend, rrecv, fin, ysend, yrecv, strecv,
    ins, pools, xs, xr, a1s, a1r, a2s, a2r, ws, wr, sts, strs, d2s, d2r, rss, rrs, yss, yrs,
):
    yh, z, x, yl, c = (lax.axis_index(a) for a in AXES)
    y = yh * 2 + yl
    tp = x * 4 + yl * 2 + c
    zb = lax.rem(z // 2, 2)

    def at_y(k):
        return {"yh": k // 2, "yl": lax.rem(k, 2)}

    def at_tp(k):
        return {"x": k // 4, "yl": lax.rem(k // 2, 2), "c": lax.rem(k, 2)}

    def add(a, k, n):
        return lax.rem(a + (k + n) % n, n)

    pool_copies = (
        pltpu.make_async_copy(kp_ref, kpool, pools.at[0]),
        pltpu.make_async_copy(vp_ref, vpool, pools.at[1]),
    )
    in_copies = [
        pltpu.make_async_copy(src, dst, ins.at[k])
        for k, (src, dst) in enumerate(
            (
                (wq_hbm, wq_ref), (wk_hbm, wk_ref), (wv_hbm, wv_ref), (gain_hbm, gain_ref),
                (h_hbm, raw), (bq_hbm, bq_ref), (bk_hbm, bk_ref), (bv_hbm, bv_ref),
            )
        )
    ]
    for copy in in_copies:
        copy.start()

    barrier = pltpu.get_barrier_semaphore()
    for d in range(1, 16):
        pl.semaphore_signal(barrier, inc=1, device_id=at_tp(add(tp, d, 16)), device_id_type=MESH)
    for d in range(1, 4):
        for k in range(4):
            pl.semaphore_signal(
                barrier,
                inc=1,
                device_id={"yh": add(yh, d, 4), "yl": k // 2, "c": k % 2},
                device_id_type=MESH,
            )
    for d in (1, -1):
        pl.semaphore_signal(barrier, inc=1, device_id={"z": add(z, d, 8)}, device_id_type=MESH)

    for copy in in_copies[:4]:
        copy.wait()
    cast_weights((yh * 8 + z) * 16 + tp, gain_ref, wq_ref, wk_ref, wv_ref, w_ref)
    in_copies[4].wait()
    h_ref[...] = raw[...].reshape(BR, KB)
    pl.semaphore_wait(barrier, 29)
    for copy in pool_copies:
        copy.start()

    y_next = (at_y(add(y, 1, 8)), at_y(add(y, -1, 8)))
    z_next = ({"z": add(z, 1, 8)}, {"z": add(z, -1, 8)})

    def x_copy(s, h, way):
        o = add(y, -(s - 1) if way == 0 else s - 1, 8)
        rows = pl.ds(RT * h, RT)
        src = h_ref.at[rows] if s == 1 else xg.at[o, rows]
        return remote(
            src, xg.at[o, rows], xs.at[way, s - 1, h], xr.at[way, s - 1, h], y_next[way]
        )

    def x_wait(s, h, way):
        o = add(y, -s if way == 0 else s, 8)
        dst = xg.at[o, pl.ds(RT * h, RT)]
        remote(dst, dst, xs.at[way, s - 1, h], xr.at[way, s - 1, h], y_next[way]).wait_recv()

    def goes(s, h, way):
        return s <= 3 or (s == 4 and h == way)

    turn = (0, 1, 3, 2)

    def goes_w(s, q, way):
        return goes(s, q // 2, way)

    def origin_w(s, way):
        o = add(z, -s if way == 0 else s, 8)
        return o, lax.rem(o // 2, 2) == c, (o // 4) * 2 + lax.rem(o, 2)

    def w_copy(s, q, way):
        _, mine, j = origin_w(s - 1, way)
        part = wz.at[j, add(x, turn[q], 4)]
        return mine, remote(
            part, part, ws.at[way, s - 1, q], wr.at[way, s - 1, q], z_next[way]
        )

    def w_step(s, q, way):
        _, mine, j = origin_w(s, way)
        part = wz.at[j, add(x, turn[q], 4)]

        @pl.when(mine)
        def _():
            remote(
                part, part, ws.at[way, s - 1, q], wr.at[way, s - 1, q], z_next[way]
            ).wait_recv()
            if goes_w(s + 1, q, way):
                w_copy(s + 1, q, way)[1].start()

    def x_step(s, h):
        for way in range(2):
            if goes(s, h, way):
                x_wait(s, h, way)
                if goes(s + 1, h, way):
                    x_copy(s + 1, h, way).start()

    def a1_copy(d):
        k = add(y, d, 8)
        return remote(w_ref.at[k], a1.at[y], a1s.at[d], a1r.at[y], at_y(k))

    for d in (4, 3, 5, 2, 6, 1, 7):
        a1_copy(d).start()
    for h in range(2):
        for way in range(2):
            x_copy(1, h, way).start()

    def st_copy(d):
        k = add(tp, d, 16)
        return remote(st_ref.at[k], strecv.at[tp], sts.at[d], strs.at[tp], at_tp(k))

    for copy in in_copies[5:]:
        copy.wait()
    fill_stats(h_ref, bq_ref, bk_ref, bv_ref, st_ref)
    for d in range(1, 16):
        st_copy(d).start()
    a1[y] = w_ref[y]
    xg[y] = h_ref[...]
    strecv[tp] = st_ref[tp]
    turns(len_ref, rope)

    for d in range(1, 8):
        k = add(y, d, 8)
        remote(a1.at[k], a1.at[k], a1s.at[d], a1r.at[k], at_y(k)).wait_recv()

    own_j = (z // 4) * 2 + lax.rem(z, 2)

    def a2_copy(d):
        k = add(x, d, 4)
        return remote(
            a1.at[pl.ds(2 * k, 2)],
            wz.at[own_j, x, :, c],
            a2s.at[d],
            a2r.at[x * 2 + c],
            {"x": k, "c": zb},
        )

    for d in (2, 1, 3):
        a2_copy(d).start()

    @pl.when(zb != c)
    def _():
        a2_copy(0).start()

    @pl.when(zb == c)
    def _():
        wz[own_j, x, :, c] = a1[pl.ds(2 * x, 2)]

    x_step(1, 0)
    x_step(1, 1)

    @pl.when(zb == c)
    def _():
        for q in range(4):
            kx = add(x, turn[q], 4)
            for kc in (c, 1 - c):
                if q == 0 and kc is c:
                    continue
                dst = wz.at[own_j, kx, :, kc]
                k = kx * 2 + kc
                remote(dst, dst, a2s.at[0], a2r.at[k], {"x": kx, "c": kc}).wait_recv()
            for way in range(2):
                w_copy(1, q, way)[1].start()

    x_step(2, 0)
    x_step(2, 1)
    for s in range(1, 5):
        for q in range(4):
            for way in range(2):
                if goes_w(s, q, way):
                    w_step(s, q, way)
        if s <= 2:
            x_step(s + 2, 0)
            x_step(s + 2, 1)

    def one_block(b, carry):
        total = jnp.zeros((BR, COLS), jnp.float32)
        for k in range(2):
            total += jnp.dot(
                xg[b * 2 + k],
                wz[2 * k : 2 * k + 2].reshape(KB, COLS),
                preferred_element_type=jnp.float32,
            )
        acc[b] = total
        return carry

    oc = 1 - c
    HR = RT // 2

    def rows_for(half, kx, kc):
        at = pl.multiple_of((kx * 2 + kc) * 24, 8)
        return acc[2 * half : 2 * half + 2, pl.ds(at, 24), :].reshape(HR, COLS)

    order = (2, 1, 3, 0)

    def d_copy(half, d):
        return remote(
            dsend.at[half, d], drecv.at[half, d], d2s.at[half, d], d2r.at[half, d], {"c": oc}
        )

    for half in range(2):
        lax.fori_loop(2 * half, 2 * half + 2, one_block, 0)
        for d in order:
            dsend[half, d] = rows_for(half, add(x, d, 4), oc).astype(jnp.bfloat16)
            d_copy(half, d).start()

    def both_cores(half, d):
        d_copy(half, d).wait_recv()
        return rows_for(half, add(x, d, 4), c) + drecv[half, d].astype(jnp.float32)

    x_next = ({"x": add(x, 1, 4)}, {"x": add(x, -1, 4)})

    def r_copy(kind, half):
        way = half if kind == 0 else (1 - half if kind == 1 else half)
        return remote(
            rsend.at[kind, half], rrecv.at[kind, half], rss.at[kind, half], rrs.at[kind, half],
            x_next[way],
        )

    for half in range(2):
        rsend[0, half] = both_cores(half, 2).astype(jnp.bfloat16)
        r_copy(0, half).start()
        rsend[1, half] = both_cores(half, 3 if half == 0 else 1).astype(jnp.bfloat16)
        r_copy(1, half).start()
    for half in range(2):
        fin[pl.ds(half * HR, HR), :] = both_cores(half, 1 if half == 0 else 3)
    for half in range(2):
        r_copy(0, half).wait_recv()
        total = fin[pl.ds(half * HR, HR), :] + rrecv[0, half].astype(jnp.float32)
        rsend[2, half] = total.astype(jnp.bfloat16)
        r_copy(2, half).start()
    fin[pl.ds(RT, 8), :] = jnp.zeros((8, COLS), jnp.float32)
    for half in range(2):
        fin[pl.ds(half * HR, HR), :] = both_cores(half, 0)
    for half in range(2):
        r_copy(1, half).wait_recv()
        fin[pl.ds(half * HR, HR), :] += rrecv[1, half].astype(jnp.float32)
    for half in range(2):
        r_copy(2, half).wait_recv()
        fin[pl.ds(half * HR, HR), :] += rrecv[2, half].astype(jnp.float32)

    def y_copy(d, dc):
        k = add(yh, d, 4)
        kc = lax.rem(c + dc, 2)
        return remote(
            ysend.at[k, kc],
            yrecv.at[y],
            yss.at[d, dc],
            yrs.at[y],
            {"yh": k, "yl": c, "c": kc},
        )

    def y_each(act):
        for d in (0, 1, 3, 2):
            for dc in range(2):
                if d == 0 and dc == 0:

                    @pl.when(yl != c)
                    def _():
                        act(y_copy(0, 0))
                else:
                    act(y_copy(d, dc))

    for k in range(4):
        for kc in range(2):
            ysend[k, kc] = fin[pl.ds(24 * k + OWN * kc, 16), :].astype(jnp.bfloat16)
    y_each(lambda copy: copy.start())

    @pl.when(yl == c)
    def _():
        yrecv[y] = ysend[yh, c]

    for d in range(1, 16):
        k = add(tp, d, 16)
        remote(strecv.at[k], strecv.at[k], sts.at[d], strs.at[k], at_tp(k)).wait_recv()
    for copy in pool_copies:
        copy.wait()

    inv = row_scale(strecv)

    def one_group(d, carry):
        kh = lax.rem(yh + jnp.where(d == 2, 3, jnp.where(d == 3, 2, d)), 4)
        for i in range(2):
            k = kh * 2 + i

            @pl.when((k != y) | (yl != c))
            def _(k=k):
                remote(
                    yrecv.at[k], yrecv.at[k], yss.at[1, 0], yrs.at[k], {"yh": add(yh, 1, 4)}
                ).wait_recv()

        attend(kh, inv, len_ref, table_ref, yrecv, strecv, rope, kpool, vpool, out_ref)
        return carry

    lax.fori_loop(0, 4, one_group, 0)

    for d in range(1, 8):
        a1_copy(d).wait_send()
    y_each(lambda copy: copy.wait_send())
    for d in range(1, 16):
        st_copy(d).wait_send()
    for d in range(1, 4):
        a2_copy(d).wait_send()

    @pl.when(zb != c)
    def _():
        a2_copy(0).wait_send()

    for half in range(2):
        for d in range(4):
            d_copy(half, d).wait_send()
        for kind in range(3):
            r_copy(kind, half).wait_send()
    for s in range(1, 5):
        for h in range(2):
            for way in range(2):
                if goes(s, h, way):
                    x_copy(s, h, way).wait_send()
    for s in range(1, 5):
        for q in range(4):
            for way in range(2):
                if goes_w(s, q, way):
                    mine, copy = w_copy(s, q, way)

                    @pl.when(mine)
                    def _(copy=copy):
                        copy.wait_send()


def on_device(
    hidden,
    norm_gain,
    w_query,
    w_key,
    w_value,
    bias_query,
    bias_key,
    bias_value,
    key_pages,
    value_pages,
    kv_lengths,
    page_table,
):
    vm = pltpu.VMEM
    dma = pltpu.SemaphoreType.DMA
    bf = jnp.bfloat16
    f32 = jnp.float32
    out = pl.pallas_call(
        step_kernel,
        out_shape=jax.ShapeDtypeStruct((ROWS, STEPS, HQ * HD), f32),
        in_specs=[pl.BlockSpec(memory_space=pltpu.SMEM)] * 2
        + [pl.BlockSpec(memory_space=pl.ANY)] * 10,
        out_specs=pl.BlockSpec(memory_space=vm),
        scratch_shapes=[
            vm((ROWS * 16, STEPS, KB), bf),
            vm((D // 128, 128), f32),
            vm((16, HQ * HD), f32),
            vm((16, KVH * HD), f32),
            vm((16, KVH * HD), f32),
            vm((2, 128), f32),
            vm((1, 32), f32),
            vm((1, 32), f32),
            vm((BR, KB), bf),
            vm((8, 16, COLS), bf),
            vm((16, 8, 128), f32),
            vm((2, 16, 128), f32),
            vm((16, KVH, PAGE, HD), bf),
            vm((16, KVH, PAGE, HD), bf),
            vm((8, BR, KB), bf),
            vm((8, 16, COLS), bf),
            vm((4, 4, 2, 2, 16, COLS), bf),
            vm((4, BR, COLS), f32),
            vm((2, 4, RT // 2, COLS), bf),
            vm((2, 4, RT // 2, COLS), bf),
            vm((3, 2, RT // 2, COLS), bf),
            vm((3, 2, RT // 2, COLS), bf),
            vm((RT + 8, COLS), f32),
            vm((4, 2, 16, COLS), bf),
            vm((8, 16, COLS), bf),
            vm((16, 8, 128), f32),
            dma((8,)), dma((2,)),
            dma((2, 4, 2)), dma((2, 4, 2)),
            dma((8,)), dma((8,)),
            dma((4,)), dma((8,)),
            dma((2, 4, 4)), dma((2, 4, 4)),
            dma((16,)), dma((16,)),
            dma((2, 4)), dma((2, 4)),
            dma((3, 2)), dma((3, 2)),
            dma((4, 2)), dma((8,)),
        ],
        compiler_params=pltpu.CompilerParams(collective_id=0, has_side_effects=True),
        name="step",
    )(
        kv_lengths,
        page_table,
        hidden,
        norm_gain.reshape(D // 128, 128),
        w_query,
        w_key,
        w_value,
        bias_query.reshape(2, 128),
        bias_key.reshape(1, 32),
        bias_value.reshape(1, 32),
        key_pages,
        value_pages,
    )
    return out.astype(bf)


def solution(mesh):
    split = Mesh(mesh.devices.reshape(4, 8, 4, 2, 2), AXES)
    both = REPLICA + TP
    in_specs = (
        P(REPLICA, None, TP),
        P(),
        P(both, None),
        P(both, None),
        P(both, None),
        P(TP),
        P(TP),
        P(TP),
        P(both, None, None, None),
        P(both, None, None, None),
        P(both),
        P(both, None),
    )
    return jax.shard_map(
        on_device, mesh=split, in_specs=in_specs, out_specs=P(both, None, None), check_vma=False
    )
```

```python
import functools

import jax
import jax.numpy as jnp
from jax import lax
from jax.experimental import pallas as pl
from jax.experimental.pallas import tpu as pltpu
from jax.sharding import Mesh
from jax.sharding import PartitionSpec as P

HD = 128
HQ = 32
KVH = 4
GROUP = HQ // KVH
PAGE = 128
MOSTP = 8
STEPS = 4
ROWS = 3
OWN = ROWS * STEPS
D = 8192
EPS = 1e-06
THETA = 1000000.0
MESH = pl.DeviceIdType.MESH
AXES = ("yh", "z", "x", "yl", "c")
TP = ("x", "yl", "c")
REPLICA = ("yh", "z")
COLS = 640
KB = 512
BR = 192
KEYS = MOSTP * PAGE + 128
RT = 96


def remote(src, dst, send, recv, where):
    return pltpu.make_async_remote_copy(
        src_ref=src, dst_ref=dst, send_sem=send, recv_sem=recv, device_id=where, device_id_type=MESH
    )


def column_of(row, shape):
    rows = lax.broadcasted_iota(jnp.int32, shape, 0)
    lanes = lax.broadcasted_iota(jnp.int32, shape, 1)
    return jnp.sum(
        jnp.where(rows == lanes, jnp.broadcast_to(row, shape), 0.0), axis=1, keepdims=True
    )


def cast_weights(block, gain_ref, wq_ref, wk_ref, wv_ref, w_ref):
    row = gain_ref[pl.ds(block // 8, 1), :]
    rows = lax.broadcasted_iota(jnp.int32, (16, 128), 0)
    lanes = lax.broadcasted_iota(jnp.int32, (16, 128), 1)
    low = lanes < HD // 2
    gain = jnp.sum(
        jnp.where(lanes == rows + lax.rem(block, 8) * 16, jnp.broadcast_to(row, (16, 128)), 0.0),
        axis=1,
        keepdims=True,
    )
    for k in range(8):
        w_ref[k, :, 0:512] = (wq_ref[:, 512 * k : 512 * k + 512] * gain).astype(jnp.bfloat16)
        tiles = slice(HD * (k // 2), HD * (k // 2) + HD)
        tk, tv = wk_ref[:, tiles] * gain, wv_ref[:, tiles] * gain
        if k % 2 == 0:
            both = jnp.where(low, tk, pltpu.roll(tv, HD // 2, 1))
        else:
            both = jnp.where(low, pltpu.roll(tk, HD // 2, 1), tv)
        w_ref[k, :, 512:640] = both.astype(jnp.bfloat16)


def fill_stats(h_ref, bq_ref, bk_ref, bv_ref, st_ref):
    wide = h_ref[...].astype(jnp.float32)
    squares = jnp.sum(wide * wide, axis=1, keepdims=True)
    of_row = lax.broadcasted_iota(jnp.int32, (BR, 128), 0)
    of_lane = lax.broadcasted_iota(jnp.int32, (BR, 128), 1)
    spread = jnp.where(lax.rem(of_row, OWN) == of_lane, squares, 0.0)
    group = lax.broadcasted_iota(jnp.int32, (16, BR), 0)
    member = lax.broadcasted_iota(jnp.int32, (16, BR), 1)
    owner = jnp.where(member // OWN == group, 1.0, 0.0)
    per_owner = jnp.dot(
        owner, spread, preferred_element_type=jnp.float32, precision=lax.Precision.HIGHEST
    )
    for k in range(16):
        st_ref[k, 0:2, :] = bq_ref[...]
        st_ref[k, 2:3, 0:32] = bk_ref[...]
        st_ref[k, 3:4, 0:32] = bv_ref[...]
        st_ref[k, 4:5, :] = per_owner[k : k + 1, :]


def turns(len_ref, rope):
    rows = lax.broadcasted_iota(jnp.int32, (16, 128), 0)
    lanes = lax.broadcasted_iota(jnp.int32, (16, 128), 1)
    row_of = rows // STEPS
    length = jnp.where(row_of == 0, len_ref[0], jnp.where(row_of == 1, len_ref[1], len_ref[2]))
    position = (length + lax.rem(rows, STEPS)).astype(jnp.float32)
    pair = lax.rem(lanes, HD // 2).astype(jnp.float32)
    freq = jnp.power(THETA, -(pair * 2.0 / HD))
    angle = position * freq
    rope[0] = jnp.cos(angle)
    sin = jnp.sin(angle)
    rope[1] = jnp.where(lanes < HD // 2, -sin, sin)


def row_scale(strecv):
    squares = jnp.sum(strecv[:, 4, :], axis=0, keepdims=True)
    return lax.rsqrt(column_of(squares, (16, 128)) * (1.0 / D) + EPS)


def attend(groups, inv, len_ref, table_ref, qkv, st, rope, kpool, vpool, score, out_ref):
    rows = lax.broadcasted_iota(jnp.int32, (16, 128), 0)
    lanes = lax.broadcasted_iota(jnp.int32, (16, 128), 1)
    keep = rows < OWN
    low = lanes < HD // 2
    cos, sin = rope[0], rope[1]
    nothing = jnp.zeros((112, HD), jnp.bfloat16)

    def made(total, bias):
        value = (total * inv + bias).astype(jnp.bfloat16).astype(jnp.float32)
        return jnp.where(keep, value, 0.0)

    def rotated(value):
        return (value * cos + pltpu.roll(value, HD // 2, 1) * sin).astype(jnp.bfloat16)

    def small_bias(kh, at):
        lane = lax.broadcasted_iota(jnp.int32, (1, 128), 1)
        out = jnp.zeros((1, 128), jnp.float32)
        for i in range(4):
            piece = st[4 * kh + i, at : at + 1, :]
            if i:
                piece = pltpu.roll(piece, 32 * i, 1)
            out = jnp.where(lane // 32 == i, piece, out)
        return out

    sel_row = lax.broadcasted_iota(jnp.int32, (32, 128), 0)
    sel_col = lax.broadcasted_iota(jnp.int32, (32, 128), 1)
    spot = lax.broadcasted_iota(jnp.int32, (32, MOSTP * PAGE), 1)
    scale = 1.0 / HD**0.5
    contract = (((1,), (1,)), ((), ()))
    chains = [(n, kh, r) for n, kh in enumerate(groups) for r in range(ROWS)]
    made_of = []
    for kh in groups:
        heads = []
        for g in range(GROUP):
            i, a = g // 4, g % 4
            total = qkv[2 * kh + i, :, a * HD : (a + 1) * HD].astype(jnp.float32)
            bias = st[2 * (2 * kh + i) + a // 2, a % 2 : a % 2 + 1, :]
            heads.append(rotated(made(total, bias)))
        t0 = qkv[2 * kh, :, 4 * HD : 5 * HD].astype(jnp.float32)
        t1 = qkv[2 * kh + 1, :, 4 * HD : 5 * HD].astype(jnp.float32)
        k_new = rotated(made(jnp.where(low, t0, pltpu.roll(t1, HD // 2, 1)), small_bias(kh, 2)))
        v_new = made(jnp.where(low, pltpu.roll(t0, HD // 2, 1), t1), small_bias(kh, 3))
        made_of.append((jnp.concatenate(heads, axis=0), k_new, v_new.astype(jnp.bfloat16)))

    queries = []
    for n, kh, r in chains:
        want = (sel_row // STEPS) * 16 + r * STEPS + lax.rem(sel_row, STEPS)
        pick = jnp.where(sel_col == want, 1.0, 0.0).astype(jnp.bfloat16)
        q = jnp.dot(pick, made_of[n][0], preferred_element_type=jnp.float32)
        queries.append(q.astype(jnp.bfloat16))
    tops = []
    for (n, kh, r), q in zip(chains, queries):
        keys = jnp.concatenate(
            [kpool[table_ref[r, m], kh] for m in range(MOSTP)] + [made_of[n][1], nothing], axis=0
        )
        raw = lax.dot_general(q, keys, contract, preferred_element_type=jnp.float32)
        cache = jnp.where(spot < len_ref[r], raw[:, : MOSTP * PAGE], -1e30)
        fresh_live = (
            (sel_col < OWN)
            & (sel_col // STEPS == r)
            & (lax.rem(sel_col, STEPS) <= lax.rem(sel_row, STEPS))
        )
        fresh = jnp.where(fresh_live, raw[:, MOSTP * PAGE :], -1e30)
        score[n * ROWS + r, :, 0 : MOSTP * PAGE] = cache
        score[n * ROWS + r, :, MOSTP * PAGE : KEYS] = fresh
        tops.append(
            jnp.maximum(
                jnp.max(cache, axis=1, keepdims=True), jnp.max(fresh, axis=1, keepdims=True)
            )
        )
    results = []
    for (n, kh, r), top in zip(chains, tops):
        weight = jnp.exp((score[n * ROWS + r] - top) * scale)
        total = jnp.sum(weight, axis=1, keepdims=True)
        vals = jnp.concatenate(
            [vpool[table_ref[r, m], kh] for m in range(MOSTP)] + [made_of[n][2], nothing], axis=0
        )
        out = jnp.dot(weight.astype(jnp.bfloat16), vals, preferred_element_type=jnp.float32)
        results.append((out, total))
    for (n, kh, r), (out, total) in zip(chains, results):
        out = (out / total).astype(jnp.bfloat16)
        for g in range(GROUP):
            at = pl.ds(pl.multiple_of(kh * GROUP * HD + g * HD, HD), HD)
            out_ref[r, :, at] = out[g * STEPS : (g + 1) * STEPS, :]


def step_kernel(
    len_hbm, table_hbm, h_hbm, gain_hbm, wq_hbm, wk_hbm, wv_hbm, bq_hbm, bk_hbm, bv_hbm, kp_ref, vp_ref,
    out_hbm,
    len_ref, table_ref, out_ref, score, raw, gain_ref, wq_ref, wk_ref, wv_ref, bq_ref, bk_ref, bv_ref, h_ref,
    w_ref, st_ref, rope, kpool, vpool,
    xg, wz, acc, dsend, drecv, rsend, rrecv, fin, ysend, yrecv, strecv,
    ins, outs, pools, xs, xr, a1s, a1r, ws, wr, sts, strs, d2s, d2r, rss, rrs, yss, yrs,
):
    yh, z, x, yl, c = (lax.axis_index(a) for a in AXES)
    y = yh * 2 + yl
    tp = x * 4 + yl * 2 + c
    zb = lax.rem(z // 2, 2)

    def at_y(k):
        return {"yh": k // 2, "yl": lax.rem(k, 2)}

    def at_tp(k):
        return {"x": k // 4, "yl": lax.rem(k // 2, 2), "c": lax.rem(k, 2)}

    def add(a, k, n):
        return lax.rem(a + lax.rem(k + n, n), n)

    pool_copies = (
        pltpu.make_async_copy(kp_ref, kpool, pools.at[0]),
        pltpu.make_async_copy(vp_ref, vpool, pools.at[1]),
    )
    in_copies = [
        pltpu.make_async_copy(src, dst, ins.at[k])
        for k, (src, dst) in enumerate(
            (
                (wq_hbm, wq_ref), (wk_hbm, wk_ref), (wv_hbm, wv_ref), (gain_hbm, gain_ref),
                (h_hbm, raw), (bq_hbm, bq_ref), (bk_hbm, bk_ref), (bv_hbm, bv_ref),
                (len_hbm, len_ref), (table_hbm, table_ref),
            )
        )
    ]
    for copy in in_copies:
        copy.start()

    barrier = pltpu.get_barrier_semaphore()
    near_x = [add(x, d, 4) for d in range(4)]
    near_yh = [add(yh, d, 4) for d in range(4)]
    near_yl, near_c = (yl, 1 - yl), (c, 1 - c)
    for k in range(1, 64):
        pl.semaphore_signal(
            barrier,
            inc=1,
            device_id={
                "yh": near_yh[k // 16],
                "x": near_x[k // 4 % 4],
                "yl": near_yl[k // 2 % 2],
                "c": near_c[k % 2],
            },
            device_id_type=MESH,
        )
    for d in (1, -1):
        pl.semaphore_signal(barrier, inc=1, device_id={"z": add(z, d, 8)}, device_id_type=MESH)

    for copy in in_copies[:4]:
        copy.wait()
    cast_weights((yh * 8 + z) * 16 + tp, gain_ref, wq_ref, wk_ref, wv_ref, w_ref)
    in_copies[4].wait()
    h_ref[...] = raw[...].reshape(BR, KB)
    pl.semaphore_wait(barrier, 65)
    for copy in pool_copies:
        copy.start()

    y_next = (at_y(add(y, 1, 8)), at_y(add(y, -1, 8)))
    z_next = ({"z": add(z, 1, 8)}, {"z": add(z, -1, 8)})

    def x_copy(s, h, way):
        o = add(y, -(s - 1) if way == 0 else s - 1, 8)
        rows = pl.ds(RT * h, RT)
        src = h_ref.at[rows] if s == 1 else xg.at[o, rows]
        return remote(
            src, xg.at[o, rows], xs.at[0], xr.at[way, s - 1, h], y_next[way]
        )

    def x_wait(s, h, way):
        o = add(y, -s if way == 0 else s, 8)
        dst = xg.at[o, pl.ds(RT * h, RT)]
        remote(dst, dst, xs.at[0], xr.at[way, s - 1, h], y_next[way]).wait_recv()

    def goes(s, h, way):
        return s <= 3 or (s == 4 and h == way)

    turn = (0, 1, 3, 2)

    def goes_w(s, q, way):
        return goes(s, q // 2, way)

    def origin_w(s, way):
        o = add(z, -s if way == 0 else s, 8)
        return o, lax.rem(o // 2, 2) == c, (o // 4) * 2 + lax.rem(o, 2)

    def w_copy(s, q, way):
        _, mine, j = origin_w(s - 1, way)
        part = wz.at[j, add(x, turn[q], 4)]
        return mine, remote(
            part, part, ws.at[way, s - 1, q], wr.at[way, s - 1, q], z_next[way]
        )

    def w_step(s, q, way):
        _, mine, j = origin_w(s, way)
        part = wz.at[j, add(x, turn[q], 4)]

        @pl.when(mine)
        def _():
            remote(
                part, part, ws.at[way, s - 1, q], wr.at[way, s - 1, q], z_next[way]
            ).wait_recv()
            if goes_w(s + 1, q, way):
                w_copy(s + 1, q, way)[1].start()

    def x_step(s, h):
        for way in range(2):
            if goes(s, h, way):
                x_wait(s, h, way)
                if goes(s + 1, h, way):
                    x_copy(s + 1, h, way).start()

    own_j = (z // 4) * 2 + lax.rem(z, 2)

    def a1_copy(d):
        k = add(y, d, 8)
        return remote(
            w_ref.at[k],
            wz.at[own_j, x, yl, c],
            a1s.at[d],
            a1r.at[tp],
            {"x": yh, "yh": k // 2, "yl": lax.rem(k, 2), "c": zb},
        )

    at_home = (x == yh) & (zb == c)
    for d in (4, 3, 5, 2, 6, 1, 7):
        a1_copy(d).start()

    @pl.when(jnp.logical_not(at_home))
    def _():
        a1_copy(0).start()

    for h in range(2):
        for way in range(2):
            x_copy(1, h, way).start()

    def st_copy(d):
        k = add(tp, d, 16)
        return remote(st_ref.at[k], strecv.at[tp], sts.at[0], strs.at[0], at_tp(k))

    for copy in in_copies[5:]:
        copy.wait()
    fill_stats(h_ref, bq_ref, bk_ref, bv_ref, st_ref)
    for d in range(1, 16):
        st_copy(d).start()

    @pl.when(at_home)
    def _():
        wz[own_j, x, yl, c] = w_ref[y]

    xg[y] = h_ref[...]
    strecv[tp] = st_ref[tp]
    turns(len_ref, rope)


    @pl.when(zb == c)
    def _():
        for q in range(4):
            kx = add(x, turn[q], 4)
            for kl in range(2):
                for kc in range(2):
                    dst = wz.at[own_j, kx, kl, kc]
                    k = kx * 4 + kl * 2 + kc

                    @pl.when(jnp.logical_not(at_home & (k == tp)))
                    def _(dst=dst, k=k, kx=kx, kc=kc):
                        remote(dst, dst, a1s.at[0], a1r.at[k], {"x": kx, "c": 1 - c}).wait_recv()

            for way in range(2):
                w_copy(1, q, way)[1].start()

    za, zl = z // 4, lax.rem(z, 2)
    held = zb == c
    far = jnp.where(zb == zl, za, 1 - za)
    parts = (
        jnp.where(held, 2 * za + zl, 2 * (1 - far) + 1 - zl),
        jnp.where(held, 2 * za + 1 - zl, zl),
        jnp.where(held, 2 * (1 - za) + 1 - zl, 2 + zl),
        jnp.where(held, 2 * (1 - za) + zl, 2 * far + 1 - zl),
    )

    def product(b, which):
        total = None
        for n in which:
            j = parts[n]
            cols = pl.ds(pl.multiple_of(lax.rem(j, 2) * 256, 256), 256)
            term = jnp.dot(
                xg[b * 2 + j // 2, :, cols],
                wz[j].reshape(256, COLS),
                preferred_element_type=jnp.float32,
            )
            total = term if total is None else total + term
        return total

    def rest(b, carry):
        acc[b] += product(b, (2, 3))
        return carry

    def w_both(s, q):
        for way in range(2):
            if goes_w(s, q, way):
                w_step(s, q, way)

    def first(d):
        b = add(yh, d, 4)
        acc[b] = product(b, (0, 1))

    for kind, s, k in (
        ("x", 1, 0), ("x", 1, 1), ("w", 1, 0), ("w", 1, 1), ("w", 1, 2), ("x", 2, 0), ("w", 1, 3),
        ("w", 2, 0), ("x", 2, 1), ("w", 2, 1), ("w", 2, 2), ("x", 3, 0), ("w", 2, 3), ("w", 3, 0),
        ("x", 3, 1), ("w", 3, 1), ("m", 0, 0), ("w", 3, 2), ("m", 0, 1), ("w", 3, 3), ("m", 0, 3),
        ("x", 4, 0), ("x", 4, 1), ("m", 0, 2), ("w", 4, 0), ("w", 4, 1), ("w", 4, 2), ("w", 4, 3),
    ):
        if kind == "x":
            x_step(s, k)
        elif kind == "w":
            w_both(s, k)
        else:
            first(k)

    oc = 1 - c
    HR = RT // 2

    def rows_for(half, kx, kc):
        at = pl.multiple_of((kx * 2 + kc) * 24, 8)
        return acc[2 * half : 2 * half + 2, pl.ds(at, 24), :].reshape(HR, COLS)

    order = (2, 1, 3, 0)

    def d_copy(half, d):
        return remote(
            dsend.at[half, d], drecv.at[half, d], d2s.at[half, d], d2r.at[half, d], {"c": oc}
        )

    for half in range(2):
        lax.fori_loop(2 * half, 2 * half + 2, rest, 0)
        for d in order:
            dsend[half, d] = rows_for(half, add(x, d, 4), oc).astype(jnp.bfloat16)
            d_copy(half, d).start()

    def both_cores(half, d):
        d_copy(half, d).wait_recv()
        return rows_for(half, add(x, d, 4), c) + drecv[half, d].astype(jnp.float32)

    x_next = ({"x": add(x, 1, 4)}, {"x": add(x, -1, 4)})

    def r_copy(kind, half):
        way = half if kind == 0 else (1 - half if kind == 1 else half)
        return remote(
            rsend.at[kind, half], rrecv.at[kind, half], rss.at[kind, half], rrs.at[kind, half],
            x_next[way],
        )

    for half in range(2):
        rsend[0, half] = both_cores(half, 2).astype(jnp.bfloat16)
        r_copy(0, half).start()
        rsend[1, half] = both_cores(half, 3 if half == 0 else 1).astype(jnp.bfloat16)
        r_copy(1, half).start()
    for half in range(2):
        fin[pl.ds(half * HR, HR), :] = both_cores(half, 1 if half == 0 else 3)
    for d in range(1, 8):
        a1_copy(d).wait_send()
    sent = st_ref.at[pl.ds(0, 15)]
    remote(sent, sent, sts.at[0], strs.at[0], at_tp(add(tp, 1, 16))).wait_send()

    @pl.when(jnp.logical_not(at_home))
    def _():
        a1_copy(0).wait_send()

    seven = xg.at[pl.ds(0, 7)]
    remote(seven, seven, xs.at[0], xr.at[0, 0, 0], y_next[0]).wait_send()
    for s in range(1, 5):
        for q in range(4):
            for way in range(2):
                if goes_w(s, q, way):
                    mine, copy = w_copy(s, q, way)

                    @pl.when(mine)
                    def _(copy=copy):
                        copy.wait_send()
    for half in range(2):
        r_copy(0, half).wait_recv()
        total = fin[pl.ds(half * HR, HR), :] + rrecv[0, half].astype(jnp.float32)
        rsend[2, half] = total.astype(jnp.bfloat16)
        r_copy(2, half).start()
    fin[pl.ds(RT, 8), :] = jnp.zeros((8, COLS), jnp.float32)
    for half in range(2):
        fin[pl.ds(half * HR, HR), :] = both_cores(half, 0)
    for half in range(2):
        r_copy(1, half).wait_recv()
        fin[pl.ds(half * HR, HR), :] += rrecv[1, half].astype(jnp.float32)
    for half in range(2):
        r_copy(2, half).wait_recv()
        fin[pl.ds(half * HR, HR), :] += rrecv[2, half].astype(jnp.float32)

    def y_copy(d, dc):
        k = add(yh, d, 4)
        kc = lax.rem(c + dc, 2)
        return remote(
            ysend.at[k, kc],
            yrecv.at[y],
            yss.at[d, dc],
            yrs.at[y],
            {"yh": k, "yl": c, "c": kc},
        )

    def y_each(act):
        for d in (0, 1, 3, 2):
            for dc in range(2):
                if d == 0 and dc == 0:

                    @pl.when(yl != c)
                    def _():
                        act(y_copy(0, 0))
                else:
                    act(y_copy(d, dc))

    for k in range(4):
        for kc in range(2):
            ysend[k, kc] = fin[pl.ds(24 * k + OWN * kc, 16), :].astype(jnp.bfloat16)
    y_each(lambda copy: copy.start())

    @pl.when(yl == c)
    def _():
        yrecv[y] = ysend[yh, c]

    fifteen = strecv.at[pl.ds(0, 15)]
    remote(fifteen, fifteen, sts.at[0], strs.at[0], at_tp(add(tp, 1, 16))).wait_recv()
    for copy in pool_copies:
        copy.wait()

    for half in range(2):
        for d in range(4):
            d_copy(half, d).wait_send()
        for kind in range(3):
            r_copy(kind, half).wait_send()
    inv = row_scale(strecv)

    def out_copy(d):
        kh = lax.rem(yh + jnp.where(d == 2, 3, jnp.where(d == 3, 2, d)), 4)
        at = pl.ds(pl.multiple_of(kh * GROUP * HD, GROUP * HD), GROUP * HD)
        return kh, pltpu.make_async_copy(
            out_ref.at[:, :, at], out_hbm.at[:, :, at], outs.at[d]
        )

    def one_pair(p, carry):
        groups = []
        for u in range(2):
            kh, _ = out_copy(2 * p + u)
            groups.append(kh)
            for i in range(2):
                k = kh * 2 + i

                @pl.when((k != y) | (yl != c))
                def _(k=k):
                    remote(
                        yrecv.at[k], yrecv.at[k], yss.at[1, 0], yrs.at[k], {"yh": add(yh, 1, 4)}
                    ).wait_recv()

        attend(groups, inv, len_ref, table_ref, yrecv, strecv, rope, kpool, vpool, score, out_ref)
        for u in range(2):
            out_copy(2 * p + u)[1].start()
        return carry

    lax.fori_loop(0, 2, one_pair, 0)
    y_each(lambda copy: copy.wait_send())
    for d in range(4):
        out_copy(d)[1].wait()


def on_device(
    hidden,
    norm_gain,
    w_query,
    w_key,
    w_value,
    bias_query,
    bias_key,
    bias_value,
    key_pages,
    value_pages,
    kv_lengths,
    page_table,
):
    vm = pltpu.VMEM
    dma = pltpu.SemaphoreType.DMA
    bf = jnp.bfloat16
    f32 = jnp.float32
    out = pl.pallas_call(
        step_kernel,
        out_shape=jax.ShapeDtypeStruct((ROWS, STEPS, HQ * HD), bf),
        in_specs=[pl.BlockSpec(memory_space=pl.ANY)] * 12,
        out_specs=pl.BlockSpec(memory_space=pl.ANY),
        scratch_shapes=[
            pltpu.SMEM((ROWS,), jnp.int32),
            pltpu.SMEM((ROWS, MOSTP), jnp.int32),
            vm((ROWS, STEPS, HQ * HD), bf),
            vm((2 * ROWS, GROUP * STEPS, KEYS), f32),
            vm((ROWS * 16, STEPS, KB), bf),
            vm((D // 128, 128), f32),
            vm((16, HQ * HD), f32),
            vm((16, KVH * HD), f32),
            vm((16, KVH * HD), f32),
            vm((2, 128), f32),
            vm((1, 32), f32),
            vm((1, 32), f32),
            vm((BR, KB), bf),
            vm((8, 16, COLS), bf),
            vm((16, 8, 128), f32),
            vm((2, 16, 128), f32),
            vm((16, KVH, PAGE, HD), bf),
            vm((16, KVH, PAGE, HD), bf),
            vm((8, BR, KB), bf),
            vm((4, 4, 2, 2, 16, COLS), bf),
            vm((4, BR, COLS), f32),
            vm((2, 4, RT // 2, COLS), bf),
            vm((2, 4, RT // 2, COLS), bf),
            vm((3, 2, RT // 2, COLS), bf),
            vm((3, 2, RT // 2, COLS), bf),
            vm((RT + 8, COLS), f32),
            vm((4, 2, 16, COLS), bf),
            vm((8, 16, COLS), bf),
            vm((16, 8, 128), f32),
            dma((10,)), dma((4,)), dma((2,)),
            dma((1,)), dma((2, 4, 2)),
            dma((8,)), dma((16,)),
            dma((2, 4, 4)), dma((2, 4, 4)),
            dma((1,)), dma((1,)),
            dma((2, 4)), dma((2, 4)),
            dma((3, 2)), dma((3, 2)),
            dma((4, 2)), dma((8,)),
        ],
        compiler_params=pltpu.CompilerParams(collective_id=0, has_side_effects=True),
        name="step",
    )(
        kv_lengths,
        page_table,
        hidden,
        norm_gain.reshape(D // 128, 128),
        w_query,
        w_key,
        w_value,
        bias_query.reshape(2, 128),
        bias_key.reshape(1, 32),
        bias_value.reshape(1, 32),
        key_pages,
        value_pages,
    )
    return out


def solution(mesh):
    split = Mesh(mesh.devices.reshape(4, 8, 4, 2, 2), AXES)
    both = REPLICA + TP
    in_specs = (
        P(REPLICA, None, TP),
        P(),
        P(both, None),
        P(both, None),
        P(both, None),
        P(TP),
        P(TP),
        P(TP),
        P(both, None, None, None),
        P(both, None, None, None),
        P(both),
        P(both, None),
    )
    return jax.shard_map(
        on_device, mesh=split, in_specs=in_specs, out_specs=P(both, None, None), check_vma=False
    )
```

```python
import functools

import jax
import jax.numpy as jnp
from jax import lax
from jax.experimental import pallas as pl
from jax.experimental.pallas import tpu as pltpu
from jax.sharding import Mesh
from jax.sharding import PartitionSpec as P

HD = 128
HQ = 32
KVH = 4
GROUP = HQ // KVH
PAGE = 128
MOSTP = 8
STEPS = 4
ROWS = 3
OWN = ROWS * STEPS
D = 8192
EPS = 1e-06
THETA = 1000000.0
MESH = pl.DeviceIdType.MESH
AXES = ("yh", "z", "x", "yl", "c")
TP = ("x", "yl", "c")
REPLICA = ("yh", "z")
COLS = 640
KB = 512
BR = 192
KEYS = MOSTP * PAGE + 128
RT = 96


def remote(src, dst, send, recv, where):
    return pltpu.make_async_remote_copy(
        src_ref=src, dst_ref=dst, send_sem=send, recv_sem=recv, device_id=where, device_id_type=MESH
    )


def column_of(row, shape):
    rows = lax.broadcasted_iota(jnp.int32, shape, 0)
    lanes = lax.broadcasted_iota(jnp.int32, shape, 1)
    return jnp.sum(
        jnp.where(rows == lanes, jnp.broadcast_to(row, shape), 0.0), axis=1, keepdims=True
    )


def cast_weights(block, gain_ref, wq_ref, wk_ref, wv_ref, w_ref):
    row = gain_ref[pl.ds(block // 8, 1), :]
    rows = lax.broadcasted_iota(jnp.int32, (16, 128), 0)
    lanes = lax.broadcasted_iota(jnp.int32, (16, 128), 1)
    low = lanes < HD // 2
    gain = jnp.sum(
        jnp.where(lanes == rows + lax.rem(block, 8) * 16, jnp.broadcast_to(row, (16, 128)), 0.0),
        axis=1,
        keepdims=True,
    )
    for k in range(8):
        w_ref[k, :, 0:512] = (wq_ref[:, 512 * k : 512 * k + 512] * gain).astype(jnp.bfloat16)
        tiles = slice(HD * (k // 2), HD * (k // 2) + HD)
        tk, tv = wk_ref[:, tiles] * gain, wv_ref[:, tiles] * gain
        if k % 2 == 0:
            both = jnp.where(low, tk, pltpu.roll(tv, HD // 2, 1))
        else:
            both = jnp.where(low, pltpu.roll(tk, HD // 2, 1), tv)
        w_ref[k, :, 512:640] = both.astype(jnp.bfloat16)


def fill_stats(h_ref, bq_ref, bk_ref, bv_ref, st_ref):
    wide = h_ref[...].astype(jnp.float32)
    squares = jnp.sum(wide * wide, axis=1, keepdims=True)
    of_row = lax.broadcasted_iota(jnp.int32, (BR, 128), 0)
    of_lane = lax.broadcasted_iota(jnp.int32, (BR, 128), 1)
    spread = jnp.where(lax.rem(of_row, OWN) == of_lane, squares, 0.0)
    group = lax.broadcasted_iota(jnp.int32, (16, BR), 0)
    member = lax.broadcasted_iota(jnp.int32, (16, BR), 1)
    owner = jnp.where(member // OWN == group, 1.0, 0.0)
    per_owner = jnp.dot(
        owner, spread, preferred_element_type=jnp.float32, precision=lax.Precision.HIGHEST
    )
    for k in range(16):
        st_ref[k, 0:2, :] = bq_ref[...]
        st_ref[k, 2:3, 0:32] = bk_ref[...]
        st_ref[k, 3:4, 0:32] = bv_ref[...]
        st_ref[k, 4:5, :] = per_owner[k : k + 1, :]


def turns(len_ref, rope):
    rows = lax.broadcasted_iota(jnp.int32, (16, 128), 0)
    lanes = lax.broadcasted_iota(jnp.int32, (16, 128), 1)
    row_of = rows // STEPS
    length = jnp.where(row_of == 0, len_ref[0], jnp.where(row_of == 1, len_ref[1], len_ref[2]))
    position = (length + lax.rem(rows, STEPS)).astype(jnp.float32)
    pair = lax.rem(lanes, HD // 2).astype(jnp.float32)
    freq = jnp.power(THETA, -(pair * 2.0 / HD))
    angle = position * freq
    rope[0] = jnp.cos(angle)
    sin = jnp.sin(angle)
    rope[1] = jnp.where(lanes < HD // 2, -sin, sin)


def row_scale(strecv):
    squares = jnp.sum(strecv[:, 4, :], axis=0, keepdims=True)
    return lax.rsqrt(column_of(squares, (16, 128)) * (1.0 / D) + EPS)


def attend(groups, inv, len_ref, table_ref, qkv, st, rope, kpool, vpool, score, out_ref):
    rows = lax.broadcasted_iota(jnp.int32, (16, 128), 0)
    lanes = lax.broadcasted_iota(jnp.int32, (16, 128), 1)
    keep = rows < OWN
    low = lanes < HD // 2
    cos, sin = rope[0], rope[1]
    nothing = jnp.zeros((112, HD), jnp.bfloat16)

    def made(total, bias):
        value = (total * inv + bias).astype(jnp.bfloat16).astype(jnp.float32)
        return jnp.where(keep, value, 0.0)

    def rotated(value):
        return (value * cos + pltpu.roll(value, HD // 2, 1) * sin).astype(jnp.bfloat16)

    def small_bias(kh, at):
        lane = lax.broadcasted_iota(jnp.int32, (1, 128), 1)
        out = jnp.zeros((1, 128), jnp.float32)
        for i in range(4):
            piece = st[4 * kh + i, at : at + 1, :]
            if i:
                piece = pltpu.roll(piece, 32 * i, 1)
            out = jnp.where(lane // 32 == i, piece, out)
        return out

    sel_row = lax.broadcasted_iota(jnp.int32, (32, 128), 0)
    sel_col = lax.broadcasted_iota(jnp.int32, (32, 128), 1)
    spot = lax.broadcasted_iota(jnp.int32, (32, MOSTP * PAGE), 1)
    scale = 1.0 / HD**0.5
    contract = (((1,), (1,)), ((), ()))
    chains = [(n, kh, r) for n, kh in enumerate(groups) for r in range(ROWS)]
    made_of = []
    for kh in groups:
        heads = []
        for g in range(GROUP):
            i, a = g // 4, g % 4
            total = qkv[2 * kh + i, :, a * HD : (a + 1) * HD].astype(jnp.float32)
            bias = st[2 * (2 * kh + i) + a // 2, a % 2 : a % 2 + 1, :]
            heads.append(rotated(made(total, bias)))
        t0 = qkv[2 * kh, :, 4 * HD : 5 * HD].astype(jnp.float32)
        t1 = qkv[2 * kh + 1, :, 4 * HD : 5 * HD].astype(jnp.float32)
        k_new = rotated(made(jnp.where(low, t0, pltpu.roll(t1, HD // 2, 1)), small_bias(kh, 2)))
        v_new = made(jnp.where(low, pltpu.roll(t0, HD // 2, 1), t1), small_bias(kh, 3))
        made_of.append((jnp.concatenate(heads, axis=0), k_new, v_new.astype(jnp.bfloat16)))

    queries = []
    for n, kh, r in chains:
        want = (sel_row // STEPS) * 16 + r * STEPS + lax.rem(sel_row, STEPS)
        pick = jnp.where(sel_col == want, 1.0, 0.0).astype(jnp.bfloat16)
        q = jnp.dot(pick, made_of[n][0], preferred_element_type=jnp.float32)
        queries.append(q.astype(jnp.bfloat16))
    tops = []
    for (n, kh, r), q in zip(chains, queries):
        keys = jnp.concatenate(
            [kpool[table_ref[r, m], kh] for m in range(MOSTP)] + [made_of[n][1], nothing], axis=0
        )
        raw = lax.dot_general(q, keys, contract, preferred_element_type=jnp.float32)
        cache = jnp.where(spot < len_ref[r], raw[:, : MOSTP * PAGE], -1e30)
        fresh_live = (
            (sel_col < OWN)
            & (sel_col // STEPS == r)
            & (lax.rem(sel_col, STEPS) <= lax.rem(sel_row, STEPS))
        )
        fresh = jnp.where(fresh_live, raw[:, MOSTP * PAGE :], -1e30)
        score[n * ROWS + r, :, 0 : MOSTP * PAGE] = cache
        score[n * ROWS + r, :, MOSTP * PAGE : KEYS] = fresh
        tops.append(
            jnp.maximum(
                jnp.max(cache, axis=1, keepdims=True), jnp.max(fresh, axis=1, keepdims=True)
            )
        )
    results = []
    for (n, kh, r), top in zip(chains, tops):
        weight = jnp.exp((score[n * ROWS + r] - top) * scale)
        total = jnp.sum(weight, axis=1, keepdims=True)
        vals = jnp.concatenate(
            [vpool[table_ref[r, m], kh] for m in range(MOSTP)] + [made_of[n][2], nothing], axis=0
        )
        out = jnp.dot(weight.astype(jnp.bfloat16), vals, preferred_element_type=jnp.float32)
        results.append((out, total))
    for (n, kh, r), (out, total) in zip(chains, results):
        out = (out / total).astype(jnp.bfloat16)
        for g in range(GROUP):
            at = pl.ds(pl.multiple_of(kh * GROUP * HD + g * HD, HD), HD)
            out_ref[r, :, at] = out[g * STEPS : (g + 1) * STEPS, :]


def step_kernel(
    len_hbm, table_hbm, h_hbm, gain_hbm, wq_hbm, wk_hbm, wv_hbm, bq_hbm, bk_hbm, bv_hbm, kp_ref, vp_ref,
    out_hbm,
    len_ref, table_ref, out_ref, score, raw, gain_ref, wq_ref, wk_ref, wv_ref, bq_ref, bk_ref, bv_ref, h_ref,
    w_ref, st_ref, rope, kpool, vpool,
    xg, wz, acc, dsend, drecv, rsend, rrecv, fin, ysend, yrecv, strecv,
    ins, outs, pools, xs, xr, a1s, a1r, ws, wr, sts, strs, d2s, d2r, rss, rrs, yss, yrs,
):
    yh, z, x, yl, c = (lax.axis_index(a) for a in AXES)
    y = yh * 2 + yl
    tp = x * 4 + yl * 2 + c
    zb = lax.rem(z // 2, 2)

    def at_y(k):
        return {"yh": k // 2, "yl": lax.rem(k, 2)}

    def at_tp(k):
        return {"x": k // 4, "yl": lax.rem(k // 2, 2), "c": lax.rem(k, 2)}

    def add(a, k, n):
        return lax.rem(a + lax.rem(k + n, n), n)

    pool_copies = (
        pltpu.make_async_copy(kp_ref, kpool, pools.at[0]),
        pltpu.make_async_copy(vp_ref, vpool, pools.at[1]),
    )
    in_copies = [
        pltpu.make_async_copy(src, dst, ins.at[k])
        for k, (src, dst) in enumerate(
            (
                (wq_hbm, wq_ref), (wk_hbm, wk_ref), (wv_hbm, wv_ref), (gain_hbm, gain_ref),
                (h_hbm, raw), (bq_hbm, bq_ref), (bk_hbm, bk_ref), (bv_hbm, bv_ref),
                (len_hbm, len_ref), (table_hbm, table_ref),
            )
        )
    ]
    for copy in in_copies:
        copy.start()

    barrier = pltpu.get_barrier_semaphore()
    near_x = [add(x, d, 4) for d in range(4)]
    near_yh = [add(yh, d, 4) for d in range(4)]
    near_yl, near_c = (yl, 1 - yl), (c, 1 - c)
    for k in range(1, 64):
        pl.semaphore_signal(
            barrier,
            inc=1,
            device_id={
                "yh": near_yh[k // 16],
                "x": near_x[k // 4 % 4],
                "yl": near_yl[k // 2 % 2],
                "c": near_c[k % 2],
            },
            device_id_type=MESH,
        )
    for d in (1, -1):
        pl.semaphore_signal(barrier, inc=1, device_id={"z": add(z, d, 8)}, device_id_type=MESH)

    for copy in in_copies[:4]:
        copy.wait()
    cast_weights((yh * 8 + z) * 16 + tp, gain_ref, wq_ref, wk_ref, wv_ref, w_ref)
    in_copies[4].wait()
    h_ref[...] = raw[...].reshape(BR, KB)
    pl.semaphore_wait(barrier, 65)
    for copy in pool_copies:
        copy.start()

    y_next = (at_y(add(y, 1, 8)), at_y(add(y, -1, 8)))
    z_next = ({"z": add(z, 1, 8)}, {"z": add(z, -1, 8)})

    def x_copy(s, h, way):
        o = add(y, -(s - 1) if way == 0 else s - 1, 8)
        rows = pl.ds(RT * h, RT)
        src = h_ref.at[rows] if s == 1 else xg.at[o, rows]
        return remote(
            src, xg.at[o, rows], xs.at[0], xr.at[way, s - 1, h], y_next[way]
        )

    def x_wait(s, h, way):
        o = add(y, -s if way == 0 else s, 8)
        dst = xg.at[o, pl.ds(RT * h, RT)]
        remote(dst, dst, xs.at[0], xr.at[way, s - 1, h], y_next[way]).wait_recv()

    def goes(s, h, way):
        return s <= 3 or (s == 4 and h == way)

    turn = (0, 1, 3, 2)

    def goes_w(s, q, way):
        return goes(s, q // 2, way)

    def origin_w(s, way):
        o = add(z, -s if way == 0 else s, 8)
        return o, lax.rem(o // 2, 2) == c, (o // 4) * 2 + lax.rem(o, 2)

    def w_copy(s, q, way):
        _, mine, j = origin_w(s - 1, way)
        part = wz.at[j * 4 + add(x, turn[q], 4)]
        return mine, remote(
            part, part, ws.at[0], wr.at[way, s - 1, q], z_next[way]
        )

    def w_step(s, q, way):
        _, mine, j = origin_w(s, way)
        part = wz.at[j * 4 + add(x, turn[q], 4)]

        @pl.when(mine)
        def _():
            remote(
                part, part, ws.at[0], wr.at[way, s - 1, q], z_next[way]
            ).wait_recv()
            if goes_w(s + 1, q, way):
                w_copy(s + 1, q, way)[1].start()

    def x_step(s, n):
        for way in range(2):
            h = n ^ way
            if goes(s, h, way):
                x_wait(s, h, way)
                if goes(s + 1, h, way):
                    x_copy(s + 1, h, way).start()

    own_j = (z // 4) * 2 + lax.rem(z, 2)

    def a1_copy(d):
        k = add(y, d, 8)
        return remote(
            w_ref.at[k],
            wz.at[own_j * 4 + x, yl, c],
            a1s.at[0 if d else 1],
            a1r.at[x],
            {"x": yh, "yh": k // 2, "yl": lax.rem(k, 2), "c": zb},
        )

    held = zb == c
    at_home = (x == yh) & held
    for d in (4, 3, 5, 2, 6, 1, 7):
        a1_copy(d).start()

    @pl.when(jnp.logical_not(at_home))
    def _():
        a1_copy(0).start()

    for h in range(2):
        for way in range(2):
            x_copy(1, h ^ way, way).start()

    def st_copy(d):
        k = add(tp, d, 16)
        return remote(st_ref.at[k], strecv.at[tp], sts.at[0], strs.at[0], at_tp(k))

    for copy in in_copies[5:]:
        copy.wait()
    fill_stats(h_ref, bq_ref, bk_ref, bv_ref, st_ref)
    for d in range(1, 16):
        st_copy(d).start()

    @pl.when(at_home)
    def _():
        wz[own_j * 4 + x, yl, c] = w_ref[y]

    xg[y] = h_ref[...]
    strecv[tp] = st_ref[tp]
    turns(len_ref, rope)


    @pl.when(held)
    def _():
        for q in (0, 2, 1, 3):
            kx = add(x, turn[q], 4)
            if q == 0:

                @pl.when(at_home)
                def _():
                    three = w_ref.at[pl.ds(0, 3)]
                    remote(three, three, a1s.at[0], a1r.at[x], {"c": 1 - c}).wait_recv()

                @pl.when(jnp.logical_not(at_home))
                def _():
                    four = wz.at[own_j * 4 + x]
                    remote(four, four, a1s.at[0], a1r.at[x], {"c": 1 - c}).wait_recv()
            else:
                four = wz.at[own_j * 4 + kx]
                remote(four, four, a1s.at[0], a1r.at[kx], {"x": kx}).wait_recv()
            w_copy(1, q, q // 2)[1].start()
        for n in range(2):
            for way in range(2):
                w_copy(1, (n + 2 - 2 * way), way)[1].start()

    za, zl = z // 4, lax.rem(z, 2)
    far = jnp.where(zb == zl, za, 1 - za)
    parts = (
        jnp.where(held, 2 * za + zl, 2 * (1 - far) + 1 - zl),
        jnp.where(held, 2 * za + 1 - zl, zl),
        jnp.where(held, 2 * (1 - za) + 1 - zl, 2 + zl),
        jnp.where(held, 2 * (1 - za) + zl, 2 * far + 1 - zl),
    )

    def product(b, which):
        total = None
        for n in which:
            j = parts[n]
            cols = pl.ds(pl.multiple_of(lax.rem(j, 2) * 256, 256), 256)
            term = jnp.dot(
                xg[b * 2 + j // 2, :, cols],
                wz[pl.ds(4 * j, 4)].reshape(256, COLS),
                preferred_element_type=jnp.float32,
            )
            total = term if total is None else total + term
        return total

    def rest(b, carry):
        acc[b] += product(b, (2, 3))
        return carry

    def w_both(s, n):
        for way in range(2):
            q = (n + 2 * way) % 4
            if goes_w(s, q, way):
                w_step(s, q, way)

    def first(d):
        b = add(yh, d, 4)
        acc[b] = product(b, (0, 1))

    for kind, s, k in (
        ("x", 1, 0), ("x", 1, 1), ("w", 1, 0), ("w", 1, 1), ("w", 1, 2), ("x", 2, 0), ("w", 1, 3),
        ("w", 2, 0), ("w", 2, 1), ("x", 2, 1), ("w", 2, 2), ("w", 2, 3), ("x", 3, 0), ("w", 3, 0),
        ("w", 3, 1), ("x", 3, 1), ("m", 0, 0), ("w", 3, 2), ("m", 0, 1), ("w", 3, 3), ("m", 0, 3),
        ("x", 4, 0), ("m", 0, 2), ("w", 4, 0), ("w", 4, 1),
    ):
        if kind == "x":
            x_step(s, k)
        elif kind == "w":
            w_both(s, k)
        else:
            first(k)

    oc = 1 - c
    HR = RT // 2

    def rows_for(half, kx, kc):
        at = pl.multiple_of((kx * 2 + kc) * 24, 8)
        return acc[2 * half : 2 * half + 2, pl.ds(at, 24), :].reshape(HR, COLS)

    order = (2, 1, 3, 0)

    def d_copy(half, d):
        return remote(
            dsend.at[half, d], drecv.at[half, d], d2s.at[0], d2r.at[half, d], {"c": oc}
        )

    for half in range(2):
        lax.fori_loop(2 * half, 2 * half + 2, rest, 0)
        for d in order:
            dsend[half, d] = rows_for(half, add(x, d, 4), oc).astype(jnp.bfloat16)
            d_copy(half, d).start()

    def both_cores(half, d):
        d_copy(half, d).wait_recv()
        return rows_for(half, add(x, d, 4), c) + drecv[half, d].astype(jnp.float32)

    x_next = ({"x": add(x, 1, 4)}, {"x": add(x, -1, 4)})

    def r_copy(kind, half, u):
        way = 1 - half if kind == 1 else half
        return remote(
            rsend.at[kind, half, u], rrecv.at[kind, half, u], rss.at[0], rrs.at[kind, half, u],
            x_next[way],
        )

    def send_half(kind, half, d):
        total = both_cores(half, d).astype(jnp.bfloat16)
        for u in range(2):
            rsend[kind, half, u] = total[24 * u : 24 * u + 24]
            r_copy(kind, half, u).start()

    for half in range(2):
        send_half(0, half, 2)
    for half in range(2):
        send_half(1, half, 3 if half == 0 else 1)
    for half in range(2):
        fin[pl.ds(half * HR, HR), :] = both_cores(half, 1 if half == 0 else 3)
    some = w_ref.at[pl.ds(0, 7)]
    remote(some, some, a1s.at[0], a1r.at[0], y_next[0]).wait_send()
    sent = st_ref.at[pl.ds(0, 15)]
    remote(sent, sent, sts.at[0], strs.at[0], at_tp(add(tp, 1, 16))).wait_send()

    @pl.when(jnp.logical_not(at_home))
    def _():
        a1_copy(0).wait_send()

    seven = xg.at[pl.ds(0, 7)]
    remote(seven, seven, xs.at[0], xr.at[0, 0, 0], y_next[0]).wait_send()
    most = wz.at[pl.ds(0, 14)]
    remote(most, most, ws.at[0], wr.at[0, 0, 0], z_next[0]).wait_send()

    def part_rows(half, u):
        return pl.ds(half * HR + 24 * u, 24)

    for u in range(2):
        for half in range(2):
            r_copy(0, half, u).wait_recv()
            total = fin[part_rows(half, u), :] + rrecv[0, half, u].astype(jnp.float32)
            rsend[2, half, u] = total.astype(jnp.bfloat16)
            r_copy(2, half, u).start()
    fin[pl.ds(RT, 8), :] = jnp.zeros((8, COLS), jnp.float32)
    for half in range(2):
        fin[pl.ds(half * HR, HR), :] = both_cores(half, 0)
    for kind in (1, 2):
        for u in range(2):
            for half in range(2):
                r_copy(kind, half, u).wait_recv()
                fin[part_rows(half, u), :] += rrecv[kind, half, u].astype(jnp.float32)

    def y_copy(d, dc):
        k = add(yh, d, 4)
        kc = lax.rem(c + dc, 2)
        return remote(
            ysend.at[k, kc],
            yrecv.at[y],
            yss.at[0 if d or dc else 1],
            yrs.at[y],
            {"yh": k, "yl": c, "c": kc},
        )

    def y_each(act):
        for d in (0, 1, 3, 2):
            for dc in range(2):
                if d == 0 and dc == 0:

                    @pl.when(yl != c)
                    def _():
                        act(y_copy(0, 0))
                else:
                    act(y_copy(d, dc))

    for k in range(4):
        for kc in range(2):
            ysend[k, kc] = fin[pl.ds(24 * k + OWN * kc, 16), :].astype(jnp.bfloat16)
    y_each(lambda copy: copy.start())

    @pl.when(yl == c)
    def _():
        yrecv[y] = ysend[yh, c]

    fifteen = strecv.at[pl.ds(0, 15)]
    remote(fifteen, fifteen, sts.at[0], strs.at[0], at_tp(add(tp, 1, 16))).wait_recv()
    for copy in pool_copies:
        copy.wait()

    remote(dsend, dsend, d2s.at[0], d2r.at[0, 0], {"c": oc}).wait_send()
    remote(rsend, rsend, rss.at[0], rrs.at[0, 0, 0], x_next[0]).wait_send()
    inv = row_scale(strecv)

    def out_copy(d):
        kh = lax.rem(yh + jnp.where(d == 2, 3, jnp.where(d == 3, 2, d)), 4)
        at = pl.ds(pl.multiple_of(kh * GROUP * HD, GROUP * HD), GROUP * HD)
        return kh, pltpu.make_async_copy(
            out_ref.at[:, :, at], out_hbm.at[:, :, at], outs.at[d]
        )

    def one_pair(p, carry):
        groups = []
        for u in range(2):
            kh, _ = out_copy(2 * p + u)
            groups.append(kh)
            for i in range(2):
                k = kh * 2 + i

                @pl.when((k != y) | (yl != c))
                def _(k=k):
                    remote(
                        yrecv.at[k], yrecv.at[k], yss.at[0], yrs.at[k], {"yh": add(yh, 1, 4)}
                    ).wait_recv()

        attend(groups, inv, len_ref, table_ref, yrecv, strecv, rope, kpool, vpool, score, out_ref)
        for u in range(2):
            out_copy(2 * p + u)[1].start()
        return carry

    lax.fori_loop(0, 2, one_pair, 0)
    rest_of = yrecv.at[pl.ds(0, 7)]
    remote(rest_of, rest_of, yss.at[0], yrs.at[0], y_next[0]).wait_send()

    @pl.when(yl != c)
    def _():
        y_copy(0, 0).wait_send()

    for d in range(4):
        out_copy(d)[1].wait()


def on_device(
    hidden,
    norm_gain,
    w_query,
    w_key,
    w_value,
    bias_query,
    bias_key,
    bias_value,
    key_pages,
    value_pages,
    kv_lengths,
    page_table,
):
    vm = pltpu.VMEM
    dma = pltpu.SemaphoreType.DMA
    bf = jnp.bfloat16
    f32 = jnp.float32
    out = pl.pallas_call(
        step_kernel,
        out_shape=jax.ShapeDtypeStruct((ROWS, STEPS, HQ * HD), bf),
        in_specs=[pl.BlockSpec(memory_space=pl.ANY)] * 12,
        out_specs=pl.BlockSpec(memory_space=pl.ANY),
        scratch_shapes=[
            pltpu.SMEM((ROWS,), jnp.int32),
            pltpu.SMEM((ROWS, MOSTP), jnp.int32),
            vm((ROWS, STEPS, HQ * HD), bf),
            vm((2 * ROWS, GROUP * STEPS, KEYS), f32),
            vm((ROWS * 16, STEPS, KB), bf),
            vm((D // 128, 128), f32),
            vm((16, HQ * HD), f32),
            vm((16, KVH * HD), f32),
            vm((16, KVH * HD), f32),
            vm((2, 128), f32),
            vm((1, 32), f32),
            vm((1, 32), f32),
            vm((BR, KB), bf),
            vm((8, 16, COLS), bf),
            vm((16, 8, 128), f32),
            vm((2, 16, 128), f32),
            vm((16, KVH, PAGE, HD), bf),
            vm((16, KVH, PAGE, HD), bf),
            vm((8, BR, KB), bf),
            vm((16, 2, 2, 16, COLS), bf),
            vm((4, BR, COLS), f32),
            vm((2, 4, RT // 2, COLS), bf),
            vm((2, 4, RT // 2, COLS), bf),
            vm((3, 2, 2, 24, COLS), bf),
            vm((3, 2, 2, 24, COLS), bf),
            vm((RT + 8, COLS), f32),
            vm((4, 2, 16, COLS), bf),
            vm((8, 16, COLS), bf),
            vm((16, 8, 128), f32),
            dma((10,)), dma((4,)), dma((2,)),
            dma((1,)), dma((2, 4, 2)),
            dma((2,)), dma((4,)),
            dma((1,)), dma((2, 4, 4)),
            dma((1,)), dma((1,)),
            dma((1,)), dma((2, 4)),
            dma((1,)), dma((3, 2, 2)),
            dma((2,)), dma((8,)),
        ],
        compiler_params=pltpu.CompilerParams(collective_id=0, has_side_effects=True),
        name="step",
    )(
        kv_lengths,
        page_table,
        hidden,
        norm_gain.reshape(D // 128, 128),
        w_query,
        w_key,
        w_value,
        bias_query.reshape(2, 128),
        bias_key.reshape(1, 32),
        bias_value.reshape(1, 32),
        key_pages,
        value_pages,
    )
    return out


def solution(mesh):
    split = Mesh(mesh.devices.reshape(4, 8, 4, 2, 2), AXES)
    both = REPLICA + TP
    in_specs = (
        P(REPLICA, None, TP),
        P(),
        P(both, None),
        P(both, None),
        P(both, None),
        P(TP),
        P(TP),
        P(TP),
        P(both, None, None, None),
        P(both, None, None, None),
        P(both),
        P(both, None),
    )
    return jax.shard_map(
        on_device, mesh=split, in_specs=in_specs, out_specs=P(both, None, None), check_vma=False
    )
```

```python
import functools

import jax
import jax.numpy as jnp
from jax import lax
from jax.experimental import pallas as pl
from jax.experimental.pallas import tpu as pltpu
from jax.sharding import Mesh
from jax.sharding import PartitionSpec as P

HD = 128
HQ = 32
KVH = 4
GROUP = HQ // KVH
PAGE = 128
MOSTP = 8
STEPS = 4
ROWS = 3
OWN = ROWS * STEPS
D = 8192
EPS = 1e-06
THETA = 1000000.0
MESH = pl.DeviceIdType.MESH
AXES = ("yh", "z", "x", "yl", "c")
TP = ("x", "yl", "c")
REPLICA = ("yh", "z")
COLS = 640
KB = 512
BR = 192
KEYS = MOSTP * PAGE + 128
RT = 96


def remote(src, dst, send, recv, where):
    return pltpu.make_async_remote_copy(
        src_ref=src, dst_ref=dst, send_sem=send, recv_sem=recv, device_id=where, device_id_type=MESH
    )


def column_of(row, shape):
    rows = lax.broadcasted_iota(jnp.int32, shape, 0)
    lanes = lax.broadcasted_iota(jnp.int32, shape, 1)
    return jnp.sum(
        jnp.where(rows == lanes, jnp.broadcast_to(row, shape), 0.0), axis=1, keepdims=True
    )


def cast_weights(block, gain_ref, wq_ref, wk_ref, wv_ref, w_ref):
    row = gain_ref[pl.ds(block // 8, 1), :]
    rows = lax.broadcasted_iota(jnp.int32, (16, 128), 0)
    lanes = lax.broadcasted_iota(jnp.int32, (16, 128), 1)
    low = lanes < HD // 2
    gain = jnp.sum(
        jnp.where(lanes == rows + lax.rem(block, 8) * 16, jnp.broadcast_to(row, (16, 128)), 0.0),
        axis=1,
        keepdims=True,
    )
    for k in range(8):
        w_ref[k, :, 0:512] = (wq_ref[:, 512 * k : 512 * k + 512] * gain).astype(jnp.bfloat16)
        tiles = slice(HD * (k // 2), HD * (k // 2) + HD)
        tk, tv = wk_ref[:, tiles] * gain, wv_ref[:, tiles] * gain
        if k % 2 == 0:
            both = jnp.where(low, tk, pltpu.roll(tv, HD // 2, 1))
        else:
            both = jnp.where(low, pltpu.roll(tk, HD // 2, 1), tv)
        w_ref[k, :, 512:640] = both.astype(jnp.bfloat16)


def fill_stats(h_ref, bq_ref, bk_ref, bv_ref, st_ref):
    wide = h_ref[...].astype(jnp.float32)
    squares = jnp.sum(wide * wide, axis=1, keepdims=True)
    of_row = lax.broadcasted_iota(jnp.int32, (BR, 128), 0)
    of_lane = lax.broadcasted_iota(jnp.int32, (BR, 128), 1)
    spread = jnp.where(lax.rem(of_row, OWN) == of_lane, squares, 0.0)
    group = lax.broadcasted_iota(jnp.int32, (16, BR), 0)
    member = lax.broadcasted_iota(jnp.int32, (16, BR), 1)
    owner = jnp.where(member // OWN == group, 1.0, 0.0)
    per_owner = jnp.dot(
        owner, spread, preferred_element_type=jnp.float32, precision=lax.Precision.HIGHEST
    )
    for k in range(16):
        st_ref[k, 0:2, :] = bq_ref[...]
        st_ref[k, 2:3, 0:32] = bk_ref[...]
        st_ref[k, 3:4, 0:32] = bv_ref[...]
        st_ref[k, 4:5, :] = per_owner[k : k + 1, :]


def turns(len_ref, rope):
    rows = lax.broadcasted_iota(jnp.int32, (16, 128), 0)
    lanes = lax.broadcasted_iota(jnp.int32, (16, 128), 1)
    row_of = rows // STEPS
    length = jnp.where(row_of == 0, len_ref[0], jnp.where(row_of == 1, len_ref[1], len_ref[2]))
    position = (length + lax.rem(rows, STEPS)).astype(jnp.float32)
    pair = lax.rem(lanes, HD // 2).astype(jnp.float32)
    freq = jnp.power(THETA, -(pair * 2.0 / HD))
    angle = position * freq
    rope[0] = jnp.cos(angle)
    sin = jnp.sin(angle)
    rope[1] = jnp.where(lanes < HD // 2, -sin, sin)


def row_scale(strecv):
    squares = jnp.sum(strecv[:, 4, :], axis=0, keepdims=True)
    return lax.rsqrt(column_of(squares, (16, 128)) * (1.0 / D) + EPS)


def attend(groups, inv, len_ref, table_ref, qkv, st, rope, kpool, vpool, score, out_ref):
    rows = lax.broadcasted_iota(jnp.int32, (16, 128), 0)
    lanes = lax.broadcasted_iota(jnp.int32, (16, 128), 1)
    keep = rows < OWN
    low = lanes < HD // 2
    cos, sin = rope[0], rope[1]
    nothing = jnp.zeros((112, HD), jnp.bfloat16)

    def made(total, bias):
        value = (total * inv + bias).astype(jnp.bfloat16).astype(jnp.float32)
        return jnp.where(keep, value, 0.0)

    def rotated(value):
        return (value * cos + pltpu.roll(value, HD // 2, 1) * sin).astype(jnp.bfloat16)

    def small_bias(kh, at):
        lane = lax.broadcasted_iota(jnp.int32, (1, 128), 1)
        out = jnp.zeros((1, 128), jnp.float32)
        for i in range(4):
            piece = st[4 * kh + i, at : at + 1, :]
            if i:
                piece = pltpu.roll(piece, 32 * i, 1)
            out = jnp.where(lane // 32 == i, piece, out)
        return out

    sel_row = lax.broadcasted_iota(jnp.int32, (32, 128), 0)
    sel_col = lax.broadcasted_iota(jnp.int32, (32, 128), 1)
    spot = lax.broadcasted_iota(jnp.int32, (32, MOSTP * PAGE), 1)
    scale = 1.0 / HD**0.5
    contract = (((1,), (1,)), ((), ()))
    chains = [(n, kh, r) for n, kh in enumerate(groups) for r in range(ROWS)]
    made_of = []
    for kh in groups:
        heads = []
        for g in range(GROUP):
            i, a = g // 4, g % 4
            total = qkv[2 * kh + i, OWN * a : OWN * a + 16, :]
            bias = st[2 * (2 * kh + i) + a // 2, a % 2 : a % 2 + 1, :]
            heads.append(rotated(made(total, bias)))
        t0 = qkv[2 * kh, 4 * OWN : 4 * OWN + 16, :]
        t1 = qkv[2 * kh + 1, 4 * OWN : 4 * OWN + 16, :]
        k_new = rotated(made(jnp.where(low, t0, pltpu.roll(t1, HD // 2, 1)), small_bias(kh, 2)))
        v_new = made(jnp.where(low, pltpu.roll(t0, HD // 2, 1), t1), small_bias(kh, 3))
        made_of.append((jnp.concatenate(heads, axis=0), k_new, v_new.astype(jnp.bfloat16)))

    queries = []
    for n, kh, r in chains:
        want = (sel_row // STEPS) * 16 + r * STEPS + lax.rem(sel_row, STEPS)
        pick = jnp.where(sel_col == want, 1.0, 0.0).astype(jnp.bfloat16)
        q = jnp.dot(pick, made_of[n][0], preferred_element_type=jnp.float32)
        queries.append(q.astype(jnp.bfloat16))
    tops = []
    for (n, kh, r), q in zip(chains, queries):
        keys = jnp.concatenate(
            [kpool[table_ref[r, m], kh] for m in range(MOSTP)] + [made_of[n][1], nothing], axis=0
        )
        raw = lax.dot_general(q, keys, contract, preferred_element_type=jnp.float32)
        cache = jnp.where(spot < len_ref[r], raw[:, : MOSTP * PAGE], -1e30)
        fresh_live = (
            (sel_col < OWN)
            & (sel_col // STEPS == r)
            & (lax.rem(sel_col, STEPS) <= lax.rem(sel_row, STEPS))
        )
        fresh = jnp.where(fresh_live, raw[:, MOSTP * PAGE :], -1e30)
        score[n * ROWS + r, :, 0 : MOSTP * PAGE] = cache
        score[n * ROWS + r, :, MOSTP * PAGE : KEYS] = fresh
        tops.append(
            jnp.maximum(
                jnp.max(cache, axis=1, keepdims=True), jnp.max(fresh, axis=1, keepdims=True)
            )
        )
    results = []
    for (n, kh, r), top in zip(chains, tops):
        weight = jnp.exp((score[n * ROWS + r] - top) * scale)
        total = jnp.sum(weight, axis=1, keepdims=True)
        vals = jnp.concatenate(
            [vpool[table_ref[r, m], kh] for m in range(MOSTP)] + [made_of[n][2], nothing], axis=0
        )
        out = jnp.dot(weight.astype(jnp.bfloat16), vals, preferred_element_type=jnp.float32)
        results.append((out, total))
    for (n, kh, r), (out, total) in zip(chains, results):
        out = (out / total).astype(jnp.bfloat16)
        for g in range(GROUP):
            at = pl.ds(pl.multiple_of(kh * GROUP * HD + g * HD, HD), HD)
            out_ref[r, :, at] = out[g * STEPS : (g + 1) * STEPS, :]


def step_kernel(
    len_hbm, table_hbm, h_hbm, gain_hbm, wq_hbm, wk_hbm, wv_hbm, bq_hbm, bk_hbm, bv_hbm, kp_ref, vp_ref,
    out_hbm,
    len_ref, table_ref, out_ref, score, raw, gain_ref, wq_ref, wk_ref, wv_ref, bq_ref, bk_ref, bv_ref, h_ref,
    w_ref, st_ref, rope, kpool, vpool,
    xg, wz, acc, dsend, drecv, rsend, rrecv, fin, ysend, yrecv, packed, strecv,
    ins, outs, pools, xs, xr, a1s, a1r, ws, wr, sts, strs, d2s, d2r, rss, rrs, yss, yrs,
):
    yh, z, x, yl, c = (lax.axis_index(a) for a in AXES)
    y = yh * 2 + yl
    tp = x * 4 + yl * 2 + c
    zb = lax.rem(z // 2, 2)

    def at_y(k):
        return {"yh": k // 2, "yl": lax.rem(k, 2)}

    def at_tp(k):
        return {"x": k // 4, "yl": lax.rem(k // 2, 2), "c": lax.rem(k, 2)}

    def add(a, k, n):
        return lax.rem(a + lax.rem(k + n, n), n)

    pool_copies = (
        pltpu.make_async_copy(kp_ref, kpool, pools.at[0]),
        pltpu.make_async_copy(vp_ref, vpool, pools.at[1]),
    )
    in_copies = [
        pltpu.make_async_copy(src, dst, ins.at[k])
        for k, (src, dst) in enumerate(
            (
                (wq_hbm, wq_ref), (wk_hbm, wk_ref), (wv_hbm, wv_ref), (gain_hbm, gain_ref),
                (h_hbm, raw), (bq_hbm, bq_ref), (bk_hbm, bk_ref), (bv_hbm, bv_ref),
                (len_hbm, len_ref), (table_hbm, table_ref),
            )
        )
    ]
    for copy in in_copies:
        copy.start()

    barrier = pltpu.get_barrier_semaphore()
    near_x = [add(x, d, 4) for d in range(4)]
    near_yh = [add(yh, d, 4) for d in range(4)]
    near_yl, near_c = (yl, 1 - yl), (c, 1 - c)
    for k in range(1, 64):
        pl.semaphore_signal(
            barrier,
            inc=1,
            device_id={
                "yh": near_yh[k // 16],
                "x": near_x[k // 4 % 4],
                "yl": near_yl[k // 2 % 2],
                "c": near_c[k % 2],
            },
            device_id_type=MESH,
        )
    for d in (1, -1):
        pl.semaphore_signal(barrier, inc=1, device_id={"z": add(z, d, 8)}, device_id_type=MESH)

    for copy in in_copies[:4]:
        copy.wait()
    cast_weights((yh * 8 + z) * 16 + tp, gain_ref, wq_ref, wk_ref, wv_ref, w_ref)
    in_copies[4].wait()
    h_ref[...] = raw[...].reshape(BR, KB)
    pl.semaphore_wait(barrier, 65)
    for copy in pool_copies:
        copy.start()

    y_next = (at_y(add(y, 1, 8)), at_y(add(y, -1, 8)))
    z_next = ({"z": add(z, 1, 8)}, {"z": add(z, -1, 8)})

    def x_copy(s, h, way):
        o = add(y, -(s - 1) if way == 0 else s - 1, 8)
        rows = pl.ds(RT * h, RT)
        src = h_ref.at[rows] if s == 1 else xg.at[o, rows]
        return remote(
            src, xg.at[o, rows], xs.at[0], xr.at[way, s - 1, h], y_next[way]
        )

    def x_wait(s, h, way):
        o = add(y, -s if way == 0 else s, 8)
        dst = xg.at[o, pl.ds(RT * h, RT)]
        remote(dst, dst, xs.at[0], xr.at[way, s - 1, h], y_next[way]).wait_recv()

    def goes(s, h, way):
        return s <= 3 or (s == 4 and h == way)

    turn = (0, 1, 3, 2)

    def goes_w(s, q, way):
        return goes(s, q // 2, way)

    def origin_w(s, way):
        o = add(z, -s if way == 0 else s, 8)
        return o, lax.rem(o // 2, 2) == c, (o // 4) * 2 + lax.rem(o, 2)

    def w_copy(s, q, way):
        _, mine, j = origin_w(s - 1, way)
        part = wz.at[j * 4 + add(x, turn[q], 4)]
        return mine, remote(
            part, part, ws.at[0], wr.at[way, s - 1, q], z_next[way]
        )

    def w_step(s, q, way):
        _, mine, j = origin_w(s, way)
        part = wz.at[j * 4 + add(x, turn[q], 4)]

        @pl.when(mine)
        def _():
            remote(
                part, part, ws.at[0], wr.at[way, s - 1, q], z_next[way]
            ).wait_recv()
            if goes_w(s + 1, q, way):
                w_copy(s + 1, q, way)[1].start()

    def x_step(s, n):
        for way in range(2):
            h = n ^ way
            if goes(s, h, way):
                x_wait(s, h, way)
                if goes(s + 1, h, way):
                    x_copy(s + 1, h, way).start()

    own_j = (z // 4) * 2 + lax.rem(z, 2)

    def a1_copy(d):
        k = add(y, d, 8)
        return remote(
            w_ref.at[k],
            wz.at[own_j * 4 + x, yl, c],
            a1s.at[0 if d else 1],
            a1r.at[x],
            {"x": yh, "yh": k // 2, "yl": lax.rem(k, 2), "c": zb},
        )

    held = zb == c
    at_home = (x == yh) & held
    for d in (4, 3, 5, 2, 6, 1, 7):
        a1_copy(d).start()

    @pl.when(jnp.logical_not(at_home))
    def _():
        a1_copy(0).start()

    for h in range(2):
        for way in range(2):
            x_copy(1, h ^ way, way).start()

    def st_copy(d):
        k = add(tp, d, 16)
        return remote(st_ref.at[k], strecv.at[tp], sts.at[0], strs.at[0], at_tp(k))

    for copy in in_copies[5:]:
        copy.wait()
    fill_stats(h_ref, bq_ref, bk_ref, bv_ref, st_ref)
    for d in range(1, 16):
        st_copy(d).start()

    @pl.when(at_home)
    def _():
        wz[own_j * 4 + x, yl, c] = w_ref[y]

    xg[y] = h_ref[...]
    strecv[tp] = st_ref[tp]
    turns(len_ref, rope)


    @pl.when(held)
    def _():
        for q in (0, 2, 1, 3):
            kx = add(x, turn[q], 4)
            if q == 0:

                @pl.when(at_home)
                def _():
                    three = w_ref.at[pl.ds(0, 3)]
                    remote(three, three, a1s.at[0], a1r.at[x], {"c": 1 - c}).wait_recv()

                @pl.when(jnp.logical_not(at_home))
                def _():
                    four = wz.at[own_j * 4 + x]
                    remote(four, four, a1s.at[0], a1r.at[x], {"c": 1 - c}).wait_recv()
            else:
                four = wz.at[own_j * 4 + kx]
                remote(four, four, a1s.at[0], a1r.at[kx], {"x": kx}).wait_recv()
            w_copy(1, q, q // 2)[1].start()
        for n in range(2):
            for way in range(2):
                w_copy(1, (n + 2 - 2 * way), way)[1].start()

    za, zl = z // 4, lax.rem(z, 2)
    far = jnp.where(zb == zl, za, 1 - za)
    parts = (
        jnp.where(held, 2 * za + zl, 2 * (1 - far) + 1 - zl),
        jnp.where(held, 2 * za + 1 - zl, zl),
        jnp.where(held, 2 * (1 - za) + 1 - zl, 2 + zl),
        jnp.where(held, 2 * (1 - za) + zl, 2 * far + 1 - zl),
    )

    def product(b, which):
        total = None
        for n in which:
            j = parts[n]
            cols = pl.ds(pl.multiple_of(lax.rem(j, 2) * 256, 256), 256)
            term = jnp.dot(
                xg[b * 2 + j // 2, :, cols],
                wz[pl.ds(4 * j, 4)].reshape(256, COLS),
                preferred_element_type=jnp.float32,
            )
            total = term if total is None else total + term
        return total

    def rest(b, carry):
        acc[b] += product(b, (2, 3))
        return carry

    def w_both(s, n):
        for way in range(2):
            q = (n + 2 * way) % 4
            if goes_w(s, q, way):
                w_step(s, q, way)

    def first(d):
        b = add(yh, d, 4)
        acc[b] = product(b, (0, 1))

    for kind, s, k in (
        ("x", 1, 0), ("x", 1, 1), ("w", 1, 0), ("w", 1, 1), ("w", 1, 2), ("x", 2, 0), ("w", 1, 3),
        ("w", 2, 0), ("w", 2, 1), ("x", 2, 1), ("w", 2, 2), ("w", 2, 3), ("x", 3, 0), ("w", 3, 0),
        ("w", 3, 1), ("x", 3, 1), ("m", 0, 0), ("w", 3, 2), ("m", 0, 1), ("w", 3, 3), ("m", 0, 3),
        ("x", 4, 0), ("m", 0, 2), ("w", 4, 0), ("w", 4, 1),
    ):
        if kind == "x":
            x_step(s, k)
        elif kind == "w":
            w_both(s, k)
        else:
            first(k)

    oc = 1 - c
    HR = RT // 2

    def rows_for(half, kx, kc):
        at = pl.multiple_of((kx * 2 + kc) * 24, 8)
        return acc[2 * half : 2 * half + 2, pl.ds(at, 24), :].reshape(HR, COLS)

    def d_copy(half, d):
        return remote(
            dsend.at[half, d], drecv.at[half, d], d2s.at[0], d2r.at[half, d], {"c": oc}
        )

    def both_cores(half, d):
        d_copy(half, d).wait_recv()
        return rows_for(half, add(x, d, 4), c) + drecv[half, d].astype(jnp.float32)

    x_next = ({"x": add(x, 1, 4)}, {"x": add(x, -1, 4)})

    def r_copy(kind, half, u):
        way = 1 - half if kind == 1 else half
        return remote(
            rsend.at[kind, half, u], rrecv.at[kind, half, u], rss.at[0], rrs.at[kind, half, u],
            x_next[way],
        )

    def send_half(kind, half, d):
        total = both_cores(half, d).astype(jnp.bfloat16)
        for u in range(2):
            rsend[kind, half, u] = total[24 * u : 24 * u + 24]
            r_copy(kind, half, u).start()

    def d_send(half, d):
        dsend[half, d] = rows_for(half, add(x, d, 4), oc).astype(jnp.bfloat16)
        d_copy(half, d).start()

    lax.fori_loop(0, 2, rest, 0)
    d_send(0, 2)
    lax.fori_loop(2, 4, rest, 0)
    for half, d in ((1, 2), (0, 3), (1, 1)):
        d_send(half, d)
    send_half(0, 0, 2)
    for half, d in ((0, 1), (1, 3)):
        d_send(half, d)
    send_half(0, 1, 2)
    for half in range(2):
        d_send(half, 0)
    for half in range(2):
        send_half(1, half, 3 if half == 0 else 1)
    for half in range(2):
        fin[pl.ds(half * HR, HR), :] = both_cores(half, 1 if half == 0 else 3)
    some = w_ref.at[pl.ds(0, 7)]
    remote(some, some, a1s.at[0], a1r.at[0], y_next[0]).wait_send()
    sent = st_ref.at[pl.ds(0, 15)]
    remote(sent, sent, sts.at[0], strs.at[0], at_tp(add(tp, 1, 16))).wait_send()

    @pl.when(jnp.logical_not(at_home))
    def _():
        a1_copy(0).wait_send()

    seven = xg.at[pl.ds(0, 7)]
    remote(seven, seven, xs.at[0], xr.at[0, 0, 0], y_next[0]).wait_send()
    most = wz.at[pl.ds(0, 14)]
    remote(most, most, ws.at[0], wr.at[0, 0, 0], z_next[0]).wait_send()

    def part_rows(half, u):
        return pl.ds(half * HR + 24 * u, 24)

    for u in range(2):
        for half in range(2):
            r_copy(0, half, u).wait_recv()
            total = fin[part_rows(half, u), :] + rrecv[0, half, u].astype(jnp.float32)
            rsend[2, half, u] = total.astype(jnp.bfloat16)
            r_copy(2, half, u).start()
    fin[pl.ds(RT, 8), :] = jnp.zeros((8, COLS), jnp.float32)
    for half in range(2):
        fin[pl.ds(half * HR, HR), :] = both_cores(half, 0)
    for kind in (1, 2):
        for u in range(2):
            for half in range(2):
                r_copy(kind, half, u).wait_recv()
                fin[part_rows(half, u), :] += rrecv[kind, half, u].astype(jnp.float32)

    def y_copy(d, dc):
        k = add(yh, d, 4)
        kc = lax.rem(c + dc, 2)
        return remote(
            ysend.at[k, kc],
            yrecv.at[y],
            yss.at[0 if d or dc else 1],
            yrs.at[y],
            {"yh": k, "yl": c, "c": kc},
        )

    def y_each(act):
        for d in (0, 1, 3, 2):
            for dc in range(2):
                if d == 0 and dc == 0:

                    @pl.when(yl != c)
                    def _():
                        act(y_copy(0, 0))
                else:
                    act(y_copy(d, dc))

    for k in range(4):
        for kc in range(2):
            for t in range(COLS // HD):
                packed[k * 2 + kc, OWN * t : OWN * (t + 1), :] = fin[
                    pl.ds(24 * k + OWN * kc, OWN), HD * t : HD * (t + 1)
                ]
            ysend[k, kc] = packed[k * 2 + kc].astype(jnp.bfloat16)
    y_each(lambda copy: copy.start())

    @pl.when(yl == c)
    def _():
        yrecv[y] = ysend[yh, c]

    fifteen = strecv.at[pl.ds(0, 15)]
    remote(fifteen, fifteen, sts.at[0], strs.at[0], at_tp(add(tp, 1, 16))).wait_recv()
    for copy in pool_copies:
        copy.wait()

    remote(dsend, dsend, d2s.at[0], d2r.at[0, 0], {"c": oc}).wait_send()
    remote(rsend, rsend, rss.at[0], rrs.at[0, 0, 0], x_next[0]).wait_send()
    inv = row_scale(strecv)

    def out_copy(d):
        kh = lax.rem(yh + jnp.where(d == 2, 3, jnp.where(d == 3, 2, d)), 4)
        at = pl.ds(pl.multiple_of(kh * GROUP * HD, GROUP * HD), GROUP * HD)
        return kh, pltpu.make_async_copy(
            out_ref.at[:, :, at], out_hbm.at[:, :, at], outs.at[d]
        )

    def one_pair(p, carry):
        groups = []
        for u in range(2):
            kh, _ = out_copy(2 * p + u)
            groups.append(kh)
            for i in range(2):
                k = kh * 2 + i

                @pl.when((k != y) | (yl != c))
                def _(k=k):
                    remote(
                        yrecv.at[k], yrecv.at[k], yss.at[0], yrs.at[k], {"yh": add(yh, 1, 4)}
                    ).wait_recv()

        for kh in groups:
            for i in range(2):
                packed[kh * 2 + i] = yrecv[kh * 2 + i].astype(jnp.float32)
        attend(groups, inv, len_ref, table_ref, packed, strecv, rope, kpool, vpool, score, out_ref)
        for u in range(2):
            out_copy(2 * p + u)[1].start()
        return carry

    lax.fori_loop(0, 2, one_pair, 0)
    rest_of = yrecv.at[pl.ds(0, 7)]
    remote(rest_of, rest_of, yss.at[0], yrs.at[0], y_next[0]).wait_send()

    @pl.when(yl != c)
    def _():
        y_copy(0, 0).wait_send()

    for d in range(4):
        out_copy(d)[1].wait()


def on_device(
    hidden,
    norm_gain,
    w_query,
    w_key,
    w_value,
    bias_query,
    bias_key,
    bias_value,
    key_pages,
    value_pages,
    kv_lengths,
    page_table,
):
    vm = pltpu.VMEM
    dma = pltpu.SemaphoreType.DMA
    bf = jnp.bfloat16
    f32 = jnp.float32
    out = pl.pallas_call(
        step_kernel,
        out_shape=jax.ShapeDtypeStruct((ROWS, STEPS, HQ * HD), bf),
        in_specs=[pl.BlockSpec(memory_space=pl.ANY)] * 12,
        out_specs=pl.BlockSpec(memory_space=pl.ANY),
        scratch_shapes=[
            pltpu.SMEM((ROWS,), jnp.int32),
            pltpu.SMEM((ROWS, MOSTP), jnp.int32),
            vm((ROWS, STEPS, HQ * HD), bf),
            vm((2 * ROWS, GROUP * STEPS, KEYS), f32),
            vm((ROWS * 16, STEPS, KB), bf),
            vm((D // 128, 128), f32),
            vm((16, HQ * HD), f32),
            vm((16, KVH * HD), f32),
            vm((16, KVH * HD), f32),
            vm((2, 128), f32),
            vm((1, 32), f32),
            vm((1, 32), f32),
            vm((BR, KB), bf),
            vm((8, 16, COLS), bf),
            vm((16, 8, 128), f32),
            vm((2, 16, 128), f32),
            vm((16, KVH, PAGE, HD), bf),
            vm((16, KVH, PAGE, HD), bf),
            vm((8, BR, KB), bf),
            vm((16, 2, 2, 16, COLS), bf),
            vm((4, BR, COLS), f32),
            vm((2, 4, RT // 2, COLS), bf),
            vm((2, 4, RT // 2, COLS), bf),
            vm((3, 2, 2, 24, COLS), bf),
            vm((3, 2, 2, 24, COLS), bf),
            vm((RT + 8, COLS), f32),
            vm((4, 2, 64, HD), bf),
            vm((8, 64, HD), bf),
            vm((8, 64, HD), f32),
            vm((16, 8, 128), f32),
            dma((10,)), dma((4,)), dma((2,)),
            dma((1,)), dma((2, 4, 2)),
            dma((2,)), dma((4,)),
            dma((1,)), dma((2, 4, 4)),
            dma((1,)), dma((1,)),
            dma((1,)), dma((2, 4)),
            dma((1,)), dma((3, 2, 2)),
            dma((2,)), dma((8,)),
        ],
        compiler_params=pltpu.CompilerParams(collective_id=0, has_side_effects=True),
        name="step",
    )(
        kv_lengths,
        page_table,
        hidden,
        norm_gain.reshape(D // 128, 128),
        w_query,
        w_key,
        w_value,
        bias_query.reshape(2, 128),
        bias_key.reshape(1, 32),
        bias_value.reshape(1, 32),
        key_pages,
        value_pages,
    )
    return out


def solution(mesh):
    split = Mesh(mesh.devices.reshape(4, 8, 4, 2, 2), AXES)
    both = REPLICA + TP
    in_specs = (
        P(REPLICA, None, TP),
        P(),
        P(both, None),
        P(both, None),
        P(both, None),
        P(TP),
        P(TP),
        P(TP),
        P(both, None, None, None),
        P(both, None, None, None),
        P(both),
        P(both, None),
    )
    return jax.shard_map(
        on_device, mesh=split, in_specs=in_specs, out_specs=P(both, None, None), check_vma=False
    )
```
